8 devices in a mesh: col: 4 (over z, y, x), row: 2 (over core).
Axes of the slice: x: 2, y: 2, z: 1, core: 2. Of those that a mesh axis runs over, the one named last changes fastest.
Arguments:
- features: bfloat16 [131072, 128], P(('row', 'col'))
- w_hidden: bfloat16 [128, 256], replicated
- w_output: bfloat16 [256, 40], replicated
- adj_cols: int32 [16, 131072], P('col', 'row')
- adj_vals: bfloat16 [16, 131072], P('col', 'row')
- adj_mask: int32 [16, 131072], P('col', 'row')
- labels: int32 [131072], P(('row', 'col'))
- train_mask: int32 [131072], P(('row', 'col'))
Outputs:
- output 1: float32 [], replicated
- output 2: float32 [128, 256], replicated
- output 3: float32 [256, 40], replicated
All inputs are finite; a program needn't handle non-finite values.
Results may differ from the reference program's by a relative error of at most 0.001.
Values are sent between devices in bfloat16 or wider.
A program may use at most 1 GiB of HBM per device.

```python
import jax
import jax.numpy as jnp
from jax import lax

NODES = 131072
FEAT = 128
HID = 256
CLS = 40
SLOTS = 16
COL_BLOCKS = 4
BLOCK_SLOTS = SLOTS // COL_BLOCKS
COL_NODES = NODES // COL_BLOCKS


def setup_inputs(seed: int = 0) -> dict:
    root_key = jax.random.key(seed)
    subkeys = jax.random.split(root_key, 8)
    adj_cols = jax.random.randint(subkeys[0], (SLOTS, NODES), 0, COL_NODES, dtype=jnp.int32)
    adj_mask = (jax.random.randint(subkeys[1], (SLOTS, NODES), 0, 4, dtype=jnp.int32) > 0).astype(jnp.int32)
    labels = jax.random.randint(subkeys[2], (NODES,), 0, CLS, dtype=jnp.int32)
    train_mask = jax.random.randint(subkeys[3], (NODES,), 0, 2, dtype=jnp.int32).at[0].set(1)
    degree = jnp.maximum(jnp.sum(adj_mask, axis=0), 1).astype(jnp.float32)
    spread = jax.random.uniform(subkeys[4], (SLOTS, NODES), jnp.float32, 0.5, 1.5)
    adj_vals = (spread * lax.rsqrt(degree)[None, :]).astype(jnp.bfloat16)
    features = jax.random.normal(subkeys[5], (NODES, FEAT), jnp.float32).astype(jnp.bfloat16)
    w_hidden = (jax.random.normal(subkeys[6], (FEAT, HID), jnp.float32) * FEAT ** -0.5).astype(jnp.bfloat16)
    w_output = (jax.random.normal(subkeys[7], (HID, CLS), jnp.float32) * HID ** -0.5).astype(jnp.bfloat16)
    return {"features": features, "w_hidden": w_hidden, "w_output": w_output, "adj_cols": adj_cols, "adj_vals": adj_vals, "adj_mask": adj_mask, "labels": labels, "train_mask": train_mask}


def gather_apply(global_cols, weights, dense):
    def slot_step(running, slot):
        col_ids, slot_w = slot
        return running + slot_w[:, None] * jnp.take(dense, col_ids, axis=0).astype(jnp.float32), None
    zero_acc = jnp.zeros((global_cols.shape[1], dense.shape[1]), jnp.float32)
    summed, _ = lax.scan(slot_step, zero_acc, (global_cols, weights))
    return summed


def scatter_apply(global_cols, weights, dense, num_out):
    dense_f = dense.astype(jnp.float32)
    def slot_step(running, slot):
        col_ids, slot_w = slot
        return running + jax.ops.segment_sum(slot_w[:, None] * dense_f, col_ids, num_segments=num_out), None
    zero_acc = jnp.zeros((num_out, dense.shape[1]), jnp.float32)
    summed, _ = lax.scan(slot_step, zero_acc, (global_cols, weights))
    return summed


def reference(features, w_hidden, w_output, adj_cols, adj_vals, adj_mask, labels, train_mask):
    offsets = (jnp.arange(SLOTS, dtype=jnp.int32) // BLOCK_SLOTS) * COL_NODES
    global_cols = adj_cols + offsets[:, None]
    weights = adj_vals.astype(jnp.float32) * adj_mask.astype(jnp.float32)
    proj_one = jnp.dot(features, w_hidden, preferred_element_type=jnp.float32).astype(jnp.bfloat16)
    z_one = gather_apply(global_cols, weights, proj_one).astype(jnp.bfloat16)
    h_one = jnp.maximum(z_one, 0)
    proj_two = jnp.dot(h_one, w_output, preferred_element_type=jnp.float32).astype(jnp.bfloat16)
    z_two = gather_apply(global_cols, weights, proj_two)
    mask_f = train_mask.astype(jnp.float32)
    train_count = jnp.maximum(jnp.sum(train_mask), 1).astype(jnp.float32)
    log_norm = jax.nn.logsumexp(z_two, axis=1)
    onehot = (labels[:, None] == jnp.arange(CLS, dtype=jnp.int32)[None, :]).astype(jnp.float32)
    picked = jnp.sum(z_two * onehot, axis=1)
    loss_mean = jnp.sum(mask_f * (log_norm - picked)) / train_count
    softmax_z = jnp.exp(z_two - log_norm[:, None])
    grad_two = ((mask_f / train_count)[:, None] * (softmax_z - onehot)).astype(jnp.bfloat16)
    back_two = scatter_apply(global_cols, weights, grad_two, NODES).astype(jnp.bfloat16)
    grad_w_output = jnp.dot(h_one.T, back_two, preferred_element_type=jnp.float32)
    dh_one = jnp.dot(back_two, w_output.T, preferred_element_type=jnp.float32)
    dz_one = jnp.where(z_one > 0, dh_one, 0.0).astype(jnp.bfloat16)
    back_one = scatter_apply(global_cols, weights, dz_one, NODES).astype(jnp.bfloat16)
    grad_w_hidden = jnp.dot(features.T, back_one, preferred_element_type=jnp.float32)
    return loss_mean, grad_w_hidden, grad_w_output
```

```python
import functools

import jax
import jax.numpy as jnp
from jax import lax
from jax.experimental import pallas as pl
from jax.experimental.pallas import tpu as pltpu
from jax.sharding import PartitionSpec as P

CONTRACT_ROWS = (((0,), (0,)), ((), ()))
CONTRACT_COLS = (((1,), (1,)), ((), ()))
LANES = 128
TILE_ROWS = 512
UNROLL = 32
CHUNK = 256
STEP_CHUNKS = 4
COL_TILE = 128
VMEM = 60 << 20


def copy_rows(idx_ref, first, count, table, stage, stage_first, width):
    def body(group, carry):
        edge = pl.multiple_of(group * UNROLL, UNROLL)
        ids = idx_ref.at[pl.ds(first + edge, UNROLL)]
        out = stage.at[pl.ds(pl.multiple_of(stage_first + width * edge, width * UNROLL), width * UNROLL)]
        for u in range(UNROLL):
            if width == 1:
                out[u, :] = table[ids[u], :]
            else:
                out[width * u:width * (u + 1), :] = table[pl.ds(pl.multiple_of(ids[u], width), width), :]
        return carry
    lax.fori_loop(0, count // UNROLL, body, 0)


def store_table(table, first, value, width):
    rows = value.shape[0]
    for part in range(width):
        piece = value[:, part * LANES:(part + 1) * LANES]
        if width == 1:
            table[pl.ds(pl.multiple_of(first, rows), rows), :] = piece
        else:
            table[pl.ds(width * first + part, rows, stride=width), :] = piece


def stream_rows(sources, buffers, sems, first_row, total, chunk, use):
    steps = total // chunk

    def copies(step, slot):
        start = pl.multiple_of(first_row + step * chunk, chunk)
        return [pltpu.make_async_copy(src.at[pl.ds(start, chunk), :], buf.at[slot], sems.at[n, slot])
                for n, (src, buf) in enumerate(zip(sources, buffers))]
    for c in copies(0, 0):
        c.start()

    def body(step, carry):
        slot = lax.rem(step, 2)
        for c in copies(step, slot):
            c.wait()

        @pl.when(step + 1 < steps)
        def _():
            for c in copies(step + 1, 1 - slot):
                c.start()
        use([buf.at[slot] for buf in buffers], step * chunk)
        return carry
    lax.fori_loop(0, steps, body, 0)


def weighted_sum(stage, w_ref, block, width):
    slots = w_ref.shape[1]
    w_rows = w_ref[0, :, block * LANES:(block + 1) * LANES]
    w_rows = jnp.concatenate([w_rows] * (8 // slots), axis=0)
    w_cols = w_rows.T
    parts = []
    for part in range(width):
        total = None
        for slot in range(slots):
            at = width * (slot * TILE_ROWS + block * LANES)
            rows = stage[pl.ds(at + part, LANES, stride=width), :] if width > 1 else stage[at:at + LANES, :]
            term = w_cols[:, slot:slot + 1] * rows
            total = term if total is None else total + term
        parts.append(total)
    return parts


def layer_one_kernel(idx_ref, w_ref, x_hbm, w_hidden, w_output, z_ref, p_ref, table, acc, stage, x_buf, sems):
    phase, tile = pl.program_id(0), pl.program_id(1)
    col_nodes = table.shape[0] // 2

    @pl.when(tile == 0)
    def _():
        def use(bufs, offset):
            for sub in range(0, x_buf.shape[1], 256):
                proj = jnp.dot(bufs[0][sub:sub + 256, :], w_hidden[...], preferred_element_type=jnp.float32)
                proj = proj.astype(jnp.bfloat16).astype(jnp.float32)
                store_table(table, offset + sub, proj, 2)
        stream_rows([x_hbm], [x_buf], sems, phase * col_nodes, col_nodes, x_buf.shape[1], use)

    copy_rows(idx_ref, 0, idx_ref.shape[0], table, stage, 0, 2)
    for block in range(TILE_ROWS // LANES):
        parts = weighted_sum(stage, w_ref, block, 2)
        rows = pl.ds(pl.multiple_of(tile * TILE_ROWS + block * LANES, LANES), LANES)

        @pl.when(phase == 0)
        def _():
            for part in range(2):
                acc[rows, part * LANES:(part + 1) * LANES] = parts[part]

        @pl.when(phase > 0)
        def _():
            for part in range(2):
                acc[rows, part * LANES:(part + 1) * LANES] += parts[part]

    @pl.when(phase == pl.num_programs(0) - 1)
    def _():
        rows = pl.ds(pl.multiple_of(tile * TILE_ROWS, TILE_ROWS), TILE_ROWS)
        z_one = acc[rows, :].astype(jnp.bfloat16)
        z_ref[...] = z_one
        h_one = jnp.maximum(z_one, 0)
        p_ref[...] = jnp.dot(h_one, w_output[...], preferred_element_type=jnp.float32).astype(jnp.bfloat16)


def layer_two_kernel(idx_ref, w_ref, p_hbm, z_ref, table, acc, stage, p_buf, sems):
    phase, tile = pl.program_id(0), pl.program_id(1)
    col_nodes = table.shape[0]

    @pl.when(tile == 0)
    def _():
        def use(bufs, offset):
            for sub in range(0, p_buf.shape[1], 256):
                store_table(table, offset + sub, bufs[0][sub:sub + 256, :].astype(jnp.float32), 1)
        stream_rows([p_hbm], [p_buf], sems, phase * col_nodes, col_nodes, p_buf.shape[1], use)

    copy_rows(idx_ref, 0, idx_ref.shape[0], table, stage, 0, 1)
    for block in range(TILE_ROWS // LANES):
        total, = weighted_sum(stage, w_ref, block, 1)
        rows = pl.ds(pl.multiple_of(tile * TILE_ROWS + block * LANES, LANES), LANES)

        @pl.when(phase == 0)
        def _():
            acc[rows, :] = total

        @pl.when(phase > 0)
        def _():
            acc[rows, :] += total

    @pl.when(phase == pl.num_programs(0) - 1)
    def _():
        rows = pl.ds(pl.multiple_of(tile * TILE_ROWS, TILE_ROWS), TILE_ROWS)
        z_ref[...] = acc[rows, :]


def segment_kernel(width, n_src, build, chunks_ref, bounds_ref, idx_ref, col_ref, w_ref, *refs):
    sources, out_hbm = refs[:n_src], refs[n_src]
    table, acc, stage, sems, out_sem = refs[n_src + 1:n_src + 6]
    buffers = refs[n_src + 6:]
    phase, step = pl.program_id(0), pl.program_id(1)
    steps = pl.num_programs(1)

    @pl.when((phase == 0) & (step == 0))
    def _():
        def zero(n, carry):
            acc[pl.ds(pl.multiple_of(n * 256, 256), 256), :] = jnp.zeros((256, acc.shape[1]), jnp.float32)
            return carry
        lax.fori_loop(0, acc.shape[0] // 256, zero, 0)

    @pl.when(step == 0)
    def _():
        build(sources, buffers, sems, phase, table)

    for part in range(STEP_CHUNKS):
        chunk = step * STEP_CHUNKS + part

        @pl.when(chunk < chunks_ref[phase])
        def _():
            copy_rows(idx_ref, part * CHUNK, CHUNK, table, stage, 0, width)
            lanes = []
            for tile in range(width):
                rows = stage[pl.ds(tile, CHUNK, stride=width), :] if width > 1 else stage[...]
                lanes.append(rows.astype(jnp.bfloat16))
            gathered = jnp.concatenate(lanes, axis=1) if width > 1 else lanes[0]
            cols = col_ref[0, :, part * CHUNK:(part + 1) * CHUNK]
            weights = w_ref[0, :, part * CHUNK:(part + 1) * CHUNK]
            where = 2 * (phase * steps * STEP_CHUNKS + chunk)

            def body(block, carry):
                local = lax.broadcasted_iota(jnp.int32, (COL_TILE, CHUNK), 0) + block * COL_TILE
                select = jnp.where(local == cols, weights, 0.0).astype(jnp.bfloat16)
                at = pl.ds(pl.multiple_of(block * COL_TILE, COL_TILE), COL_TILE)
                acc[at, :] += jnp.dot(select, gathered, preferred_element_type=jnp.float32)
                return carry
            lax.fori_loop(bounds_ref[where], bounds_ref[where + 1] + 1, body, 0)

    @pl.when((phase == pl.num_programs(0) - 1) & (step == steps - 1))
    def _():
        copy = pltpu.make_async_copy(acc, out_hbm, out_sem)
        copy.start()
        copy.wait()


def build_plain(sources, buffers, sems, phase, table):
    rows = table.shape[0]

    def use(bufs, offset):
        for sub in range(0, bufs[0].shape[0], 256):
            store_table(table, offset + sub, bufs[0][sub:sub + 256, :].astype(jnp.float32), 1)
    stream_rows(sources, buffers, sems, phase * rows, rows, buffers[0].shape[1], use)


def build_dz(sources, buffers, sems, phase, table):
    z_hbm, b_hbm, w_out = sources
    rows = table.shape[0] // 2

    def use(bufs, offset):
        for sub in range(0, bufs[0].shape[0], 256):
            z_one = bufs[0][sub:sub + 256, :]
            back = bufs[1][sub:sub + 256, :]
            dh_one = lax.dot_general(back, w_out[...], CONTRACT_COLS, preferred_element_type=jnp.float32)
            dz_one = jnp.where(z_one.astype(jnp.float32) > 0, dh_one, 0.0).astype(jnp.bfloat16)
            store_table(table, offset + sub, dz_one.astype(jnp.float32), 2)
    stream_rows([z_hbm, b_hbm], buffers, sems, phase * rows, rows, buffers[0].shape[1], use)


def params():
    return pltpu.CompilerParams(vmem_limit_bytes=VMEM, dimension_semantics=("arbitrary", "arbitrary"))


def layer_one(idx, weights, x_all, w_hidden, w_out_pad):
    phases, slots, rows = weights.shape
    nodes, feat = x_all.shape
    tiles = rows // TILE_ROWS
    hid = w_hidden.shape[1]
    last = phases - 1
    whole = pl.BlockSpec(memory_space=pltpu.VMEM)
    return pl.pallas_call(
        layer_one_kernel,
        grid=(phases, tiles),
        in_specs=[
            pl.BlockSpec((slots * TILE_ROWS,), lambda k, t: (k * tiles + t,), memory_space=pltpu.SMEM),
            pl.BlockSpec((1, slots, TILE_ROWS), lambda k, t: (k, 0, t)),
            pl.BlockSpec(memory_space=pl.ANY), whole, whole],
        out_specs=[
            pl.BlockSpec((TILE_ROWS, hid), lambda k, t: (jnp.where(k == last, t, 0), 0)),
            pl.BlockSpec((TILE_ROWS, LANES), lambda k, t: (jnp.where(k == last, t, 0), 0))],
        out_shape=[jax.ShapeDtypeStruct((rows, hid), jnp.bfloat16), jax.ShapeDtypeStruct((rows, LANES), jnp.bfloat16)],
        scratch_shapes=[
            pltpu.VMEM((2 * nodes // phases, LANES), jnp.float32), pltpu.VMEM((rows, hid), jnp.float32),
            pltpu.VMEM((2 * slots * TILE_ROWS, LANES), jnp.float32), pltpu.VMEM((2, 2048, feat), jnp.bfloat16),
            pltpu.SemaphoreType.DMA((1, 2))],
        compiler_params=params(),
        cost_estimate=pl.CostEstimate(flops=3 * 10**11, bytes_accessed=10**8, transcendentals=0),
        name="layer_one")(idx, weights, x_all, w_hidden, w_out_pad)


def layer_two(idx, weights, p_all):
    phases, slots, rows = weights.shape
    tiles = rows // TILE_ROWS
    last = phases - 1
    return pl.pallas_call(
        layer_two_kernel,
        grid=(phases, tiles),
        in_specs=[
            pl.BlockSpec((slots * TILE_ROWS,), lambda k, t: (k * tiles + t,), memory_space=pltpu.SMEM),
            pl.BlockSpec((1, slots, TILE_ROWS), lambda k, t: (k, 0, t)),
            pl.BlockSpec(memory_space=pl.ANY)],
        out_specs=pl.BlockSpec((TILE_ROWS, LANES), lambda k, t: (jnp.where(k == last, t, 0), 0)),
        out_shape=jax.ShapeDtypeStruct((rows, LANES), jnp.float32),
        scratch_shapes=[
            pltpu.VMEM((p_all.shape[0] // phases, LANES), jnp.float32), pltpu.VMEM((rows, LANES), jnp.float32),
            pltpu.VMEM((slots * TILE_ROWS, LANES), jnp.float32), pltpu.VMEM((2, 2048, LANES), jnp.bfloat16),
            pltpu.SemaphoreType.DMA((1, 2))],
        compiler_params=params(),
        cost_estimate=pl.CostEstimate(flops=3 * 10**11, bytes_accessed=10**8, transcendentals=0),
        name="layer_two")(idx, weights, p_all)


def segment_product(name, build, chunks, bounds, idx, cols, weights, sources, specs, buffers, num_out, width, rows):
    phases, edges = cols.shape
    per_step = CHUNK * STEP_CHUNKS
    steps = edges // per_step
    tile_spec = pl.BlockSpec((1, 1, per_step), lambda p, t, *_: (p * steps + t, 0, 0))
    grid_spec = pltpu.PrefetchScalarGridSpec(
        num_scalar_prefetch=2,
        grid=(phases, steps),
        in_specs=[pl.BlockSpec((per_step,), lambda p, t, *_: (p * steps + t,), memory_space=pltpu.SMEM),
                  tile_spec, tile_spec, *specs],
        out_specs=pl.BlockSpec(memory_space=pl.ANY),
        scratch_shapes=[
            pltpu.VMEM((width * rows, LANES), jnp.float32), pltpu.VMEM((num_out, width * LANES), jnp.float32),
            pltpu.VMEM((width * CHUNK, LANES), jnp.float32), pltpu.SemaphoreType.DMA((len(buffers), 2)),
            pltpu.SemaphoreType.DMA, *buffers])
    return pl.pallas_call(
        functools.partial(segment_kernel, width, len(sources), build),
        grid_spec=grid_spec,
        out_shape=jax.ShapeDtypeStruct((num_out, width * LANES), jnp.float32),
        compiler_params=params(),
        cost_estimate=pl.CostEstimate(flops=3 * 10**11, bytes_accessed=10**8, transcendentals=0),
        name=name)(chunks, bounds, (idx * width).reshape(-1), cols.reshape(phases * steps, 1, per_step),
                   weights.reshape(phases * steps, 1, per_step), *sources)


def solution(mesh):
    row_size = mesh.shape["row"]
    col_size = mesh.shape["col"]
    both_axes = ("row", "col")
    swap = [(0, 1), (1, 0)]

    def device_step(feat_blk, w_hidden, w_output, cols_blk, vals_blk, mask_blk, labels_blk, train_blk):
        row_i, col_j = lax.axis_index("row"), lax.axis_index("col")
        blk_nodes = feat_blk.shape[0]
        col_nodes = blk_nodes * row_size
        slots = cols_blk.shape[0]
        classes = w_output.shape[1]
        any_spec = pl.BlockSpec(memory_space=pl.ANY)
        whole = pl.BlockSpec(memory_space=pltpu.VMEM)
        weights = vals_blk.astype(jnp.float32) * mask_blk.astype(jnp.float32)
        w_out_pad = jnp.pad(w_output, ((0, 0), (0, LANES - classes)))

        x_all = lax.all_gather(feat_blk, both_axes, axis=0, tiled=True)
        own_cols = lax.all_to_all(cols_blk, "col", split_axis=1, concat_axis=0, tiled=True)
        own_w = lax.all_to_all(vals_blk * mask_blk.astype(jnp.bfloat16), "col", split_axis=1, concat_axis=0, tiled=True)
        own_w = own_w.astype(jnp.float32).reshape(col_size, slots, blk_nodes)
        own_cols = own_cols.reshape(col_size, slots, blk_nodes // TILE_ROWS, TILE_ROWS).transpose(0, 2, 1, 3).reshape(-1)

        first_half = 1 - row_i
        turned = jnp.bitwise_xor(cols_blk, first_half * blk_nodes)
        row_ids = lax.broadcasted_iota(jnp.int32, (slots, col_size, blk_nodes), 2)
        valid = mask_blk.reshape(slots, col_size, blk_nodes) > 0
        keys = jnp.where(valid, turned.reshape(slots, col_size, blk_nodes), col_nodes) * blk_nodes + row_ids
        keys = keys.transpose(1, 0, 2).reshape(col_size, slots * blk_nodes)
        edge_w = weights.reshape(slots, col_size, blk_nodes).transpose(1, 0, 2).reshape(col_size, slots * blk_nodes)
        keys, edge_w = lax.sort((keys, edge_w), dimension=1, num_keys=1, is_stable=False)
        edge_cols, edge_rows = keys // blk_nodes, keys % blk_nodes
        chunked = edge_cols.reshape(col_size, -1, CHUNK)
        low = chunked[:, :, 0] // COL_TILE
        high = jnp.max(jnp.where(chunked < col_nodes, chunked, 0), axis=2) // COL_TILE
        bounds = jnp.stack([low, high], axis=2).reshape(-1)
        chunks = jnp.sum((chunked[:, :, 0] < col_nodes).astype(jnp.int32), axis=1)

        z_one, proj_two = layer_one(own_cols * 2, own_w, x_all, w_hidden, w_out_pad)
        p_all = lax.all_gather(proj_two, both_axes, axis=0, tiled=True)
        z_all = lax.all_gather(z_one, "col", axis=0, tiled=True)
        z_two = layer_two(own_cols, own_w, p_all)[:, :classes]

        mask_f = train_blk.astype(jnp.float32)
        train_count = jnp.maximum(lax.psum(jnp.sum(train_blk), both_axes), 1).astype(jnp.float32)
        log_norm = jax.nn.logsumexp(z_two, axis=1)
        onehot = (labels_blk[:, None] == jnp.arange(classes, dtype=jnp.int32)[None, :]).astype(jnp.float32)
        picked = jnp.sum(z_two * onehot, axis=1)
        loss_mean = lax.psum(jnp.sum(mask_f * (log_norm - picked)), both_axes) / train_count
        softmax_z = jnp.exp(z_two - log_norm[:, None])
        grad_two = ((mask_f / train_count)[:, None] * (softmax_z - onehot)).astype(jnp.bfloat16)
        grad_two = jnp.pad(grad_two, ((0, 0), (0, LANES - classes)))
        grad_rows = lax.all_gather(grad_two, "col", axis=0, tiled=True)

        part_two = segment_product(
            "back_two", build_plain, chunks, bounds, edge_rows, edge_cols, edge_w, [grad_rows], [any_spec],
            [pltpu.VMEM((2, 2048, LANES), jnp.bfloat16)], col_nodes, 1, blk_nodes)
        other = lax.ppermute(part_two[:blk_nodes], "row", swap)
        back_two = (part_two[blk_nodes:] + other).astype(jnp.bfloat16)
        back_all = lax.all_gather(back_two, ("col", "row"), axis=0, tiled=True)
        back_rows = lax.dynamic_slice_in_dim(back_all, row_i * col_size * blk_nodes, col_size * blk_nodes, 0)
        back_own = lax.dynamic_slice_in_dim(back_rows, col_j * blk_nodes, blk_nodes, 0)
        h_one = jnp.maximum(z_one, 0)
        grad_w_output = lax.dot_general(h_one, back_own, CONTRACT_ROWS, preferred_element_type=jnp.float32)[:, :classes]

        part_one = segment_product(
            "back_one", build_dz, chunks, bounds, edge_rows, edge_cols, edge_w, [z_all, back_rows, w_out_pad],
            [any_spec, any_spec, whole],
            [pltpu.VMEM((2, 1024, 2 * LANES), jnp.bfloat16), pltpu.VMEM((2, 1024, LANES), jnp.bfloat16)],
            col_nodes, 2, blk_nodes)
        other = lax.ppermute(part_one[:blk_nodes], "row", swap)
        back_one = (part_one[blk_nodes:] + other).astype(jnp.bfloat16)
        feat_src = lax.dynamic_slice_in_dim(x_all, (col_j * row_size + row_i) * blk_nodes, blk_nodes, 0)
        grad_w_hidden = lax.dot_general(feat_src, back_one, CONTRACT_ROWS, preferred_element_type=jnp.float32)
        grad_w_hidden = lax.psum(grad_w_hidden, both_axes)
        grad_w_output = lax.psum(grad_w_output, both_axes)
        return loss_mean, grad_w_hidden, grad_w_output

    node_spec = P(("row", "col"), None)
    label_spec = P(("row", "col"))
    adj_spec = P("col", "row")
    return jax.shard_map(device_step, mesh=mesh, in_specs=(node_spec, P(), P(), adj_spec, adj_spec, adj_spec, label_spec, label_spec), out_specs=(P(), P(), P()), check_vma=False)
```

```python
import functools

import jax
import jax.numpy as jnp
from jax import lax
from jax.experimental import pallas as pl
from jax.experimental.pallas import tpu as pltpu
from jax.sharding import PartitionSpec as P

CONTRACT_ROWS = (((0,), (0,)), ((), ()))
CONTRACT_COLS = (((1,), (1,)), ((), ()))
LANES = 128
SUB_ROWS = 256
STEP_SUBS = 4
BUF_SUBS = 2
CHUNK = 256
BUF_CHUNKS = 4
STEP_CHUNKS = 8
WINDOW = 256
PACK = 3
VMEM = 60 << 20


def copy_row(ids, e, table, stage, at, width):
    if width == 1:
        stage[at, :] = table[ids[e], :]
    else:
        stage[width * at:width * (at + 1), :] = table[pl.ds(pl.multiple_of(ids[e], width), width), :]


def index_copy(idx_hbm, ids, sems, buf, step):
    size = ids[buf].shape[0]
    start = pl.multiple_of((step * len(ids) + buf) * size, size)
    return pltpu.make_async_copy(idx_hbm.at[pl.ds(start, size)], ids[buf], sems.at[buf])


def start_next(idx_hbm, ids, sems, buf, step, total):
    @pl.when(step + 1 < total)
    def _():
        index_copy(idx_hbm, ids, sems, buf, step + 1).start()


def store_table(table, first, value, width):
    rows = value.shape[0]
    for part in range(width):
        piece = value[:, part * LANES:(part + 1) * LANES]
        if width == 1:
            table[pl.ds(pl.multiple_of(first, rows), rows), :] = piece
        else:
            table[pl.ds(width * first + part, rows, stride=width), :] = piece


def stream_rows(sources, buffers, sems, first_row, total, chunk, use, sem_row=0):
    steps = total // chunk

    def copies(step, slot):
        start = pl.multiple_of(first_row + step * chunk, chunk)
        return [pltpu.make_async_copy(src.at[pl.ds(start, chunk), :], buf.at[slot], sems.at[sem_row + n, slot])
                for n, (src, buf) in enumerate(zip(sources, buffers))]
    for c in copies(0, 0):
        c.start()

    def body(step, carry):
        slot = lax.rem(step, 2)
        for c in copies(step, slot):
            c.wait()

        @pl.when(step + 1 < steps)
        def _():
            for c in copies(step + 1, 1 - slot):
                c.start()
        use([buf.at[slot] for buf in buffers], step * chunk)
        return carry
    lax.fori_loop(0, steps, body, 0)


def weighted_sum(stage, w_ref, sub, block, width):
    slots = w_ref.shape[1]
    first = sub * SUB_ROWS + block * LANES
    w_rows = w_ref[0, :, first:first + LANES]
    w_cols = jnp.concatenate([w_rows] * (8 // slots), axis=0).T
    parts = [None] * width
    for slot in range(slots):
        column = jnp.broadcast_to(w_cols[:, slot:slot + 1], (LANES, LANES))
        at = width * (slot * SUB_ROWS + block * LANES)
        for part in range(width):
            rows = stage[pl.ds(at + part, LANES, stride=width), :] if width > 1 else stage[at:at + LANES, :]
            term = column * rows
            parts[part] = term if slot == 0 else parts[part] + term
    return parts


def forward_step(idx_hbm, w_ref, table, acc, ids, stages, idx_sems, width):
    phase, tile = pl.program_id(0), pl.program_id(1)
    step = phase * pl.num_programs(1) + tile
    total = pl.num_programs(0) * pl.num_programs(1)
    slots = w_ref.shape[1]
    blocks = SUB_ROWS // LANES
    first_row = tile * STEP_SUBS * SUB_ROWS

    @pl.when(step == 0)
    def _():
        for buf in range(len(ids)):
            index_copy(idx_hbm, ids, idx_sems, buf, step).start()

    def add(sub, block):
        parts = weighted_sum(stages[sub % len(stages)], w_ref, sub, block, width)
        rows = pl.ds(pl.multiple_of(first_row + sub * SUB_ROWS + block * LANES, LANES), LANES)
        for part in range(width):
            acc[rows, part * LANES:(part + 1) * LANES] += parts[part]

    @pl.when(phase == 0)
    def _():
        rows = pl.ds(pl.multiple_of(first_row, STEP_SUBS * SUB_ROWS), STEP_SUBS * SUB_ROWS)
        acc[rows, :] = jnp.zeros((STEP_SUBS * SUB_ROWS, acc.shape[1]), jnp.float32)

    edges = slots * SUB_ROWS
    for sub in range(STEP_SUBS):
        buf, part = sub // BUF_SUBS, sub % BUF_SUBS
        if part == 0:
            index_copy(idx_hbm, ids, idx_sems, buf, step).wait()
        for block in range(blocks):
            for e in range(block * edges // blocks, (block + 1) * edges // blocks):
                copy_row(ids[buf], part * edges + e, table, stages[sub % len(stages)], e, width)
            if sub > 0:
                add(sub - 1, block)
        if part == BUF_SUBS - 1:
            start_next(idx_hbm, ids, idx_sems, buf, step, total)
    for block in range(blocks):
        add(STEP_SUBS - 1, block)


def layer_one_kernel(idx_hbm, w_ref, x_hbm, w_hidden, w_output, z_ref, p_ref, table, acc, ids_a, ids_b, stage_a, stage_b, x_buf,
                     sems, idx_sems):
    phase, tile = pl.program_id(0), pl.program_id(1)
    col_nodes = table.shape[0] // 2

    @pl.when(tile == 0)
    def _():
        def use(bufs, offset):
            for sub in range(0, x_buf.shape[1], 256):
                proj = jnp.dot(bufs[0][sub:sub + 256, :], w_hidden[...], preferred_element_type=jnp.float32)
                proj = proj.astype(jnp.bfloat16).astype(jnp.float32)
                store_table(table, offset + sub, proj, 2)
        stream_rows([x_hbm], [x_buf], sems, phase * col_nodes, col_nodes, x_buf.shape[1], use)

    forward_step(idx_hbm, w_ref, table, acc, [ids_a, ids_b], [stage_a, stage_b], idx_sems, 2)

    @pl.when(phase == pl.num_programs(0) - 1)
    def _():
        size = STEP_SUBS * SUB_ROWS
        z_one = acc[pl.ds(pl.multiple_of(tile * size, size), size), :].astype(jnp.bfloat16)
        z_ref[...] = z_one
        h_one = jnp.maximum(z_one, 0)
        p_ref[...] = jnp.dot(h_one, w_output[...], preferred_element_type=jnp.float32).astype(jnp.bfloat16)


def unpack_table(table, p_hbm, p_buf, sems, first_block, blocks, nodes, sem_row=0):
    chunk = p_buf.shape[1]
    packed = packed_rows(nodes)
    for block in range(blocks):
        def use(bufs, offset):
            value = bufs[0][...].astype(jnp.float32)
            for q in range(PACK):
                turned = value if q == 0 else pltpu.roll(value, LANES - q * pack_lanes(), 1)
                first = pl.multiple_of(block * nodes + q * packed + offset, 16)
                table[pl.ds(first, chunk), :] = turned.astype(table.dtype)
        stream_rows([p_hbm], [p_buf], sems, (first_block + block) * packed, packed, chunk, use, sem_row)


def pack_lanes():
    return LANES // PACK // 8 * 8


def packed_rows(nodes):
    return -(-nodes // (PACK * 96)) * 96


def pack_nodes(values):
    nodes = values.shape[0]
    packed = packed_rows(nodes)
    values = jnp.pad(values, ((0, PACK * packed - nodes), (0, pack_lanes() - values.shape[1])))
    parts = [values[q * packed:(q + 1) * packed] for q in range(PACK)]
    return jnp.pad(jnp.concatenate(parts, axis=1), ((0, 0), (0, LANES - PACK * pack_lanes())))


def layer_two_kernel(nodes, idx_hbm, w_ref, p_hbm, z_ref, table, acc, ids_a, ids_b, stage_a, stage_b, p_buf, sems, idx_sems):
    phase, tile = pl.program_id(0), pl.program_id(1)

    @pl.when(tile == 0)
    def _():
        unpack_table(table, p_hbm, p_buf, sems, phase * 2, 2, nodes)

    forward_step(idx_hbm, w_ref, table, acc, [ids_a, ids_b], [stage_a, stage_b], idx_sems, 1)

    @pl.when(phase == pl.num_programs(0) - 1)
    def _():
        size = STEP_SUBS * SUB_ROWS
        z_ref[...] = acc[pl.ds(pl.multiple_of(tile * size, size), size), :]


def segment_kernel(width, n_src, build, active_ref, over_ref, base_ref, last_ref, idx_hbm, col_ref, w_ref, *refs):
    sources, out_hbm = refs[:n_src], refs[n_src]
    table, acc, ids_a, ids_b, ids_c, stage_a, stage_b, sems, idx_sems, out_sem = refs[n_src + 1:n_src + 11]
    buffers = refs[n_src + 11:]
    ids, stages = [ids_a, ids_b], [stage_a, stage_b]
    phase, tile = pl.program_id(0), pl.program_id(1)
    steps = pl.num_programs(1)
    step = phase * steps + tile
    total = pl.num_programs(0) * steps

    @pl.when(step == 0)
    def _():
        for buf in range(len(ids)):
            index_copy(idx_hbm, ids, idx_sems, buf, step).start()

        def zero(n, carry):
            acc[pl.ds(pl.multiple_of(n * 256, 256), 256), :] = jnp.zeros((256, acc.shape[1]), jnp.float32)
            return carry
        lax.fori_loop(0, acc.shape[0] // 256, zero, 0)

    @pl.when(tile == 0)
    def _():
        build(sources, buffers, sems, phase, table)

    def gathered(stage):
        lanes = []
        for part in range(width):
            rows = stage[pl.ds(part, CHUNK, stride=width), :] if width > 1 else stage[...]
            lanes.append(rows.astype(jnp.bfloat16))
        return jnp.concatenate(lanes, axis=1) if width > 1 else lanes[0]

    def product(cols, weights, rows, base):
        local = lax.broadcasted_iota(jnp.int32, (WINDOW, CHUNK), 0)
        select = jnp.where(local == cols - base, weights, 0.0).astype(jnp.bfloat16)
        acc[pl.ds(pl.multiple_of(base, 8), WINDOW), :] += jnp.dot(select, rows, preferred_element_type=jnp.float32)

    def add(chunk):
        part = slice(chunk * CHUNK, (chunk + 1) * CHUNK)
        base = base_ref[step * STEP_CHUNKS + chunk]
        product(col_ref[0, :, part], w_ref[0, :, part], gathered(stages[chunk % 2]), base)

    active = tile < active_ref[phase]

    @pl.when(active)
    def _():
        for chunk in range(STEP_CHUNKS):
            buf, part = chunk // BUF_CHUNKS, chunk % BUF_CHUNKS
            if part == 0:
                index_copy(idx_hbm, ids, idx_sems, buf, step).wait()
            for e in range(CHUNK):
                copy_row(ids[buf], part * CHUNK + e, table, stages[chunk % 2], e, width)
            if chunk > 0:
                add(chunk - 1)
            if part == BUF_CHUNKS - 1:
                start_next(idx_hbm, ids, idx_sems, buf, step, total)
        add(STEP_CHUNKS - 1)

    @pl.when(jnp.logical_not(active))
    def _():
        for buf in range(len(ids)):
            index_copy(idx_hbm, ids, idx_sems, buf, step).wait()
            start_next(idx_hbm, ids, idx_sems, buf, step, total)

    @pl.when(active & (over_ref[step] > 0))
    def _():
        size = STEP_CHUNKS * CHUNK
        copy = pltpu.make_async_copy(idx_hbm.at[pl.ds(pl.multiple_of(step * size, size), size)], ids_c, out_sem)
        copy.start()
        copy.wait()
        for chunk in range(STEP_CHUNKS):
            base, last = base_ref[step * STEP_CHUNKS + chunk], last_ref[step * STEP_CHUNKS + chunk]

            @pl.when(last >= base + WINDOW)
            def _():
                def fetch(e, carry):
                    copy_row(ids_c, chunk * CHUNK + e, table, stage_a, 0, width)
                    if width == 1:
                        stage_b[pl.ds(e, 1), :] = stage_a[0:1, :]
                    else:
                        stage_b[pl.ds(width * e, width), :] = stage_a[0:width, :]
                    return carry
                lax.fori_loop(0, CHUNK, fetch, 0)
                part = slice(chunk * CHUNK, (chunk + 1) * CHUNK)
                cols, weights = col_ref[0, :, part], w_ref[0, :, part]
                rows = gathered(stage_b)
                end = acc.shape[0] - WINDOW

                def more(window, carry):
                    start = base + window * WINDOW
                    fresh = jnp.where(cols >= start, weights, 0.0)
                    product(cols, fresh, rows, jnp.minimum(start, end))
                    return carry
                lax.fori_loop(1, (last - base) // WINDOW + 1, more, 0)

    @pl.when(step == total - 1)
    def _():
        copy = pltpu.make_async_copy(acc, out_hbm, out_sem)
        copy.start()
        copy.wait()


def build_packed(nodes, sources, buffers, sems, phase, table):
    unpack_table(table, sources[0], buffers[0], sems, phase, 1, nodes)


def build_dz(nodes, sources, buffers, sems, phase, table):
    z_hbm, b_hbm, w_out = sources
    z_buf, b_buf, back = buffers
    unpack_table(back, b_hbm, b_buf, sems, phase, 1, nodes, 1)

    def use(bufs, offset):
        for sub in range(0, z_buf.shape[1], 256):
            z_one = bufs[0][sub:sub + 256, :]
            back_two = back[pl.ds(pl.multiple_of(offset + sub, 256), 256), :]
            dh_one = lax.dot_general(back_two, w_out[...], CONTRACT_COLS, preferred_element_type=jnp.float32)
            dz_one = jnp.where(z_one.astype(jnp.float32) > 0, dh_one, 0.0).astype(jnp.bfloat16)
            store_table(table, offset + sub, dz_one.astype(jnp.float32), 2)
    stream_rows([z_hbm], [z_buf], sems, phase * nodes, nodes, z_buf.shape[1], use)


def params():
    return pltpu.CompilerParams(vmem_limit_bytes=VMEM, dimension_semantics=("arbitrary", "arbitrary"))


def forward_specs(weights, last):
    slots = weights.shape[1]
    rows = STEP_SUBS * SUB_ROWS
    w_spec = pl.BlockSpec((1, slots, rows), lambda k, t: (k, 0, t))

    def out_spec(width):
        return pl.BlockSpec((rows, width), lambda k, t: (jnp.where(k == last, t, 0), 0))
    ids = pltpu.SMEM((BUF_SUBS * slots * SUB_ROWS,), jnp.int32)
    return w_spec, out_spec, [ids, ids]


def layer_one(idx, weights, x_all, w_hidden, w_out_pad):
    phases, slots, rows = weights.shape
    nodes, feat = x_all.shape
    hid = w_hidden.shape[1]
    whole = pl.BlockSpec(memory_space=pltpu.VMEM)
    any_spec = pl.BlockSpec(memory_space=pl.ANY)
    w_spec, out_spec, ids = forward_specs(weights, phases - 1)
    stage = pltpu.VMEM((2 * slots * SUB_ROWS, LANES), jnp.float32)
    return pl.pallas_call(
        layer_one_kernel,
        grid=(phases, rows // (STEP_SUBS * SUB_ROWS)),
        in_specs=[any_spec, w_spec, any_spec, whole, whole],
        out_specs=[out_spec(hid), out_spec(LANES)],
        out_shape=[jax.ShapeDtypeStruct((rows, hid), jnp.bfloat16), jax.ShapeDtypeStruct((rows, LANES), jnp.bfloat16)],
        scratch_shapes=[
            pltpu.VMEM((2 * nodes // phases, LANES), jnp.float32), pltpu.VMEM((rows, hid), jnp.float32),
            *ids, stage, stage, pltpu.VMEM((2, 2048, feat), jnp.bfloat16),
            pltpu.SemaphoreType.DMA((1, 2)), pltpu.SemaphoreType.DMA((2,))],
        compiler_params=params(),
        cost_estimate=pl.CostEstimate(flops=2 * 10**11, bytes_accessed=10**8, transcendentals=0),
        name="layer_one")(idx, weights, x_all, w_hidden, w_out_pad)


def layer_two(idx, weights, p_all):
    phases, slots, rows = weights.shape
    any_spec = pl.BlockSpec(memory_space=pl.ANY)
    w_spec, out_spec, ids = forward_specs(weights, phases - 1)
    stage = pltpu.VMEM((slots * SUB_ROWS, LANES), jnp.float32)
    return pl.pallas_call(
        functools.partial(layer_two_kernel, rows),
        grid=(phases, rows // (STEP_SUBS * SUB_ROWS)),
        in_specs=[any_spec, w_spec, any_spec],
        out_specs=out_spec(LANES),
        out_shape=jax.ShapeDtypeStruct((rows, LANES), jnp.float32),
        scratch_shapes=[
            pltpu.VMEM((2 * rows + 128, LANES), jnp.float32), pltpu.VMEM((rows, LANES), jnp.float32),
            *ids, stage, stage, pltpu.VMEM((2, packed_rows(rows) // 6, LANES), jnp.bfloat16),
            pltpu.SemaphoreType.DMA((1, 2)), pltpu.SemaphoreType.DMA((2,))],
        compiler_params=params(),
        cost_estimate=pl.CostEstimate(flops=2 * 10**11, bytes_accessed=10**8, transcendentals=0),
        name="layer_two")(idx, weights, p_all)


def segment_product(name, build, plan, sources, specs, buffers, num_out, width, rows):
    idx, cols, weights, scalars = plan
    phases, edges = cols.shape
    per_step = CHUNK * STEP_CHUNKS
    steps = edges // per_step
    any_spec = pl.BlockSpec(memory_space=pl.ANY)
    tile_spec = pl.BlockSpec((1, 1, per_step), lambda p, t, *_: (p * steps + t, 0, 0))
    ids = pltpu.SMEM((BUF_CHUNKS * CHUNK,), jnp.int32)
    stage = pltpu.VMEM((width * CHUNK, LANES), jnp.float32)
    grid_spec = pltpu.PrefetchScalarGridSpec(
        num_scalar_prefetch=len(scalars),
        grid=(phases, steps),
        in_specs=[any_spec, tile_spec, tile_spec, *specs],
        out_specs=any_spec,
        scratch_shapes=[
            pltpu.VMEM((width * rows + (128 if width == 1 else 0), LANES), jnp.float32),
            pltpu.VMEM((num_out, width * LANES), jnp.float32),
            ids, ids, pltpu.SMEM((per_step,), jnp.int32), stage, stage,
            pltpu.SemaphoreType.DMA((len(buffers), 2)), pltpu.SemaphoreType.DMA((2,)), pltpu.SemaphoreType.DMA, *buffers])
    return pl.pallas_call(
        functools.partial(segment_kernel, width, len(sources), functools.partial(build, rows)),
        grid_spec=grid_spec,
        out_shape=jax.ShapeDtypeStruct((num_out, width * LANES), jnp.float32),
        compiler_params=params(),
        cost_estimate=pl.CostEstimate(flops=2 * 10**11, bytes_accessed=10**8, transcendentals=0),
        name=name)(*scalars, (idx * width).reshape(-1), cols.reshape(phases * steps, 1, per_step),
                   weights.reshape(phases * steps, 1, per_step), *sources)


def sorted_edges(cols_blk, mask_blk, vals_blk, col_blocks, blk_nodes, turn):
    slots = cols_blk.shape[0]
    col_nodes = 2 * blk_nodes
    row_ids = lax.broadcasted_iota(jnp.int32, (slots, col_blocks, blk_nodes), 2)
    valid = mask_blk.reshape(slots, col_blocks, blk_nodes) > 0
    turned = jnp.bitwise_xor(cols_blk, turn).reshape(slots, col_blocks, blk_nodes)
    keys = jnp.where(valid, turned, col_nodes) * blk_nodes + row_ids
    weights = jnp.where(valid, vals_blk.reshape(slots, col_blocks, blk_nodes).astype(jnp.float32), 0.0)
    keys = keys.transpose(1, 0, 2).reshape(col_blocks, slots * blk_nodes)
    weights = weights.transpose(1, 0, 2).reshape(col_blocks, slots * blk_nodes)
    keys, weights = lax.sort((keys, weights), dimension=1, num_keys=1, is_stable=False)
    cols, rows = keys // blk_nodes, keys % blk_nodes
    chunked = cols.reshape(-1, CHUNK)
    base = jnp.minimum(chunked[:, 0] // 8 * 8, col_nodes - WINDOW)
    last = jnp.max(jnp.where(chunked < col_nodes, chunked, -1), axis=1)
    over = jnp.max((last >= base + WINDOW).astype(jnp.int32).reshape(-1, STEP_CHUNKS), axis=1)
    count = jnp.sum(mask_blk.reshape(slots, col_blocks, blk_nodes), axis=(0, 2))
    active = (count + STEP_CHUNKS * CHUNK - 1) // (STEP_CHUNKS * CHUNK)
    return rows, cols, weights, (active, over, base, last)


def solution(mesh):
    row_size = mesh.shape["row"]
    col_size = mesh.shape["col"]
    both_axes = ("row", "col")
    swap = [(0, 1), (1, 0)]

    def device_step(feat_blk, w_hidden, w_output, cols_blk, vals_blk, mask_blk, labels_blk, train_blk):
        row_i, col_j = lax.axis_index("row"), lax.axis_index("col")
        blk_nodes = feat_blk.shape[0]
        col_nodes = blk_nodes * row_size
        packed = packed_rows(blk_nodes)
        slots = cols_blk.shape[0]
        classes = w_output.shape[1]
        any_spec = pl.BlockSpec(memory_space=pl.ANY)
        whole = pl.BlockSpec(memory_space=pltpu.VMEM)
        w_out_pad = jnp.pad(w_output, ((0, 0), (0, LANES - classes)))

        x_all = lax.all_gather(feat_blk, both_axes, axis=0, tiled=True)
        own_cols = lax.all_to_all(cols_blk, "col", split_axis=1, concat_axis=0, tiled=True)
        own_w = lax.all_to_all(vals_blk * mask_blk.astype(jnp.bfloat16), "col", split_axis=1, concat_axis=0, tiled=True)
        own_w = own_w.astype(jnp.float32).reshape(col_size, slots, blk_nodes)
        own_cols = own_cols.reshape(col_size, slots, -1, STEP_SUBS, SUB_ROWS).transpose(0, 2, 3, 1, 4).reshape(-1)
        train_count = jnp.maximum(lax.psum(jnp.sum(train_blk), both_axes), 1).astype(jnp.float32)

        plan = sorted_edges(cols_blk, mask_blk, vals_blk, col_size, blk_nodes, (1 - row_i) * blk_nodes)
        x_all, plan, train_count = lax.optimization_barrier((x_all, plan, train_count))

        z_one, proj_two = layer_one(own_cols * 2, own_w, x_all, w_hidden, w_out_pad)
        p_all = lax.all_gather(pack_nodes(proj_two[:, :classes]), both_axes, axis=0, tiled=True)
        z_one, p_all = lax.optimization_barrier((z_one, p_all))
        z_all = lax.all_gather(z_one, "col", axis=0, tiled=True)
        z_two = layer_two(own_cols, own_w, p_all)[:, :classes]

        mask_f = train_blk.astype(jnp.float32)
        log_norm = jax.nn.logsumexp(z_two, axis=1)
        onehot = (labels_blk[:, None] == jnp.arange(classes, dtype=jnp.int32)[None, :]).astype(jnp.float32)
        picked = jnp.sum(z_two * onehot, axis=1)
        loss_mean = jnp.sum(mask_f * (log_norm - picked)) / train_count
        softmax_z = jnp.exp(z_two - log_norm[:, None])
        grad_two = ((mask_f / train_count)[:, None] * (softmax_z - onehot)).astype(jnp.bfloat16)
        z_all, grad_two = lax.optimization_barrier((z_all, grad_two))
        grad_rows = lax.all_gather(pack_nodes(grad_two), "col", axis=0, tiled=True)

        row_buf = pltpu.VMEM((2, packed // 6, LANES), jnp.bfloat16)
        part_two = segment_product(
            "back_two", build_packed, plan, [grad_rows], [any_spec], [row_buf], col_nodes, 1, blk_nodes)
        other = lax.ppermute(part_two[:blk_nodes], "row", swap)
        back_two = (part_two[blk_nodes:] + other).astype(jnp.bfloat16)
        back_all = lax.all_gather(pack_nodes(back_two[:, :classes]), ("col", "row"), axis=0, tiled=True)
        back_rows = lax.dynamic_slice_in_dim(back_all, row_i * col_size * packed, col_size * packed, 0)
        back_own = lax.dynamic_slice_in_dim(back_rows, col_j * packed, packed, 0)
        back_own = jnp.concatenate([back_own[:, q * pack_lanes():q * pack_lanes() + classes] for q in range(PACK)], axis=0)[:blk_nodes]
        h_one = jnp.maximum(z_one, 0)
        grad_w_output = lax.dot_general(h_one, back_own, CONTRACT_ROWS, preferred_element_type=jnp.float32)

        part_one = segment_product(
            "back_one", build_dz, plan, [z_all, back_rows, w_out_pad], [any_spec, any_spec, whole],
            [pltpu.VMEM((2, 1024, 2 * LANES), jnp.bfloat16), row_buf,
             pltpu.VMEM((blk_nodes + 128, LANES), jnp.bfloat16)],
            col_nodes, 2, blk_nodes)
        other = lax.ppermute(part_one[:blk_nodes], "row", swap)
        back_one = (part_one[blk_nodes:] + other).astype(jnp.bfloat16)
        feat_src = lax.dynamic_slice_in_dim(x_all, (col_j * row_size + row_i) * blk_nodes, blk_nodes, 0)
        grad_w_hidden = lax.dot_general(feat_src, back_one, CONTRACT_ROWS, preferred_element_type=jnp.float32)
        loss_mean, grad_w_hidden, grad_w_output = lax.psum((loss_mean, grad_w_hidden, grad_w_output), both_axes)
        return loss_mean, grad_w_hidden, grad_w_output

    node_spec = P(("row", "col"), None)
    label_spec = P(("row", "col"))
    adj_spec = P("col", "row")
    return jax.shard_map(device_step, mesh=mesh, in_specs=(node_spec, P(), P(), adj_spec, adj_spec, adj_spec, label_spec, label_spec), out_specs=(P(), P(), P()), check_vma=False)
```

```python
import functools

import jax
import jax.numpy as jnp
from jax import lax
from jax.experimental import pallas as pl
from jax.experimental.pallas import tpu as pltpu
from jax.sharding import PartitionSpec as P


CONTRACT_ROWS = (((0,), (0,)), ((), ()))
CONTRACT_COLS = (((1,), (1,)), ((), ()))
LANES = 128
SUB_ROWS = 256
STEP_SUBS = 4
PIECE_ROWS = 32
PIECES = 8
BUF_SUBS = 1
CHUNK = 256
BUF_CHUNKS = 2
STEP_CHUNKS = 16
WINDOW = 256
PACK = 3
INNER = 4
VMEM = 63 << 20


def copy_row(ids, e, table, stage, at, width):
    if width == 1:
        stage[at, :] = table[ids[e], :]
    else:
        stage[width * at:width * (at + 1), :] = table[pl.ds(pl.multiple_of(ids[e], width), width), :]


def index_copy(idx_hbm, ids, sems, buf, step):
    size = ids[buf].shape[0]
    start = pl.multiple_of((step * len(ids) + buf) * size, size)
    return pltpu.make_async_copy(idx_hbm.at[pl.ds(start, size)], ids[buf], sems.at[buf])


def start_next(idx_hbm, ids, sems, buf, following, total):
    @pl.when(following < total)
    def _():
        index_copy(idx_hbm, ids, sems, buf, following).start()


def store_table(table, first, value, width):
    rows = value.shape[0]
    for part in range(width):
        piece = value[:, part * LANES:(part + 1) * LANES]
        if width == 1:
            table[pl.ds(pl.multiple_of(first, rows), rows), :] = piece
        else:
            table[pl.ds(width * first + part, rows, stride=width), :] = piece


def stream_rows(source, buffer, sems, phase, phases, total, use):
    slots, chunk = buffer.shape[0], buffer.shape[1]
    steps = total // chunk
    assert steps % slots == 0

    def copy(step, slot):
        start = pl.multiple_of(phase * total + step * chunk, 16)
        return pltpu.make_async_copy(source.at[pl.ds(start, chunk), :], buffer.at[slot], sems.at[slot])

    @pl.when(phase == 0)
    def _():
        for slot in range(slots):
            copy(slot, slot).start()

    def body(group, carry):
        for slot in range(slots):
            step = group * slots + slot
            copy(step, slot).wait()
            use(buffer.at[slot], step * chunk)

            @pl.when((step + slots < steps) | (phase + 1 < phases))
            def _():
                copy(step + slots, slot).start()
        return carry

    lax.fori_loop(0, steps // slots, body, 0)


def weight_columns(w_ref, first):
    w_rows = w_ref[0, :, pl.ds(pl.multiple_of(first, LANES), LANES)]
    return jnp.concatenate([w_rows] * (8 // w_ref.shape[1]), axis=0).T


def weighted_sum(stage, w_cols, slots, first, size, width):
    parts = [None] * width
    inside = first % LANES
    for slot in range(slots):
        column = jnp.broadcast_to(w_cols[inside:inside + size, slot:slot + 1], (size, LANES))
        at = width * (slot * SUB_ROWS + first)
        for part in range(width):
            rows = stage[pl.ds(at + part, size, stride=width), :] if width > 1 else stage[at:at + size, :]
            term = column * rows
            parts[part] = term if slot == 0 else parts[part] + term
    return parts


def forward_step(idx_hbm, w_ref, table, acc, ids, stages, idx_sems, width):
    phase, tile = pl.program_id(0), pl.program_id(1)
    per_phase = pl.num_programs(1) * INNER
    total = pl.num_programs(0) * per_phase
    slots = w_ref.shape[1]
    edges = slots * SUB_ROWS
    pieces = SUB_ROWS // PIECE_ROWS
    step_rows = STEP_SUBS * SUB_ROWS

    @pl.when((phase == 0) & (tile == 0))
    def _():
        for buf in range(len(ids)):
            index_copy(idx_hbm, ids, idx_sems, buf, 0).start()

    def inner(n, carry):
        step = phase * per_phase + tile * INNER + n
        first_row = pl.multiple_of((tile * INNER + n) * step_rows, step_rows)

        @pl.when(phase == 0)
        def _():
            acc[pl.ds(first_row, step_rows), :] = jnp.zeros((step_rows, acc.shape[1]), jnp.float32)

        for sub in range(STEP_SUBS + 1):
            buf, part = sub // BUF_SUBS, sub % BUF_SUBS
            if part == 0 and sub < STEP_SUBS:
                index_copy(idx_hbm, ids, idx_sems, buf, step).wait()
            for piece in range(pieces):
                first = piece * PIECE_ROWS
                if sub > 0 and first % LANES == 0:
                    w_cols = weight_columns(w_ref, n * step_rows + (sub - 1) * SUB_ROWS + first)
                if sub < STEP_SUBS:
                    for e in range(piece * edges // pieces, (piece + 1) * edges // pieces):
                        copy_row(ids[buf], part * edges + e, table, stages[sub % len(stages)], e, width)
                if sub > 0:
                    parts = weighted_sum(stages[(sub - 1) % len(stages)], w_cols, slots, first, PIECE_ROWS, width)
                    rows = pl.ds(pl.multiple_of(first_row + (sub - 1) * SUB_ROWS + first, PIECE_ROWS), PIECE_ROWS)
                    for lane in range(width):
                        acc[rows, lane * LANES:(lane + 1) * LANES] += parts[lane]
            if part == BUF_SUBS - 1 and sub < STEP_SUBS:
                start_next(idx_hbm, ids, idx_sems, buf, step + 1, total)
        return carry

    lax.fori_loop(0, INNER, inner, 0)


def finish_rows(acc, use):
    tile = pl.program_id(1)
    size = INNER * STEP_SUBS * SUB_ROWS

    def body(n, carry):
        at = pl.multiple_of(n * 256, 256)
        use(pl.ds(at, 256), acc[pl.ds(pl.multiple_of(tile * size + at, 256), 256), :])
        return carry

    lax.fori_loop(0, size // 256, body, 0)


def layer_one_kernel(idx_hbm, w_ref, x_hbm, w_hidden, w_output, z_ref, p_ref, table, acc, ids_a, ids_b, ids_c, ids_d, stage_a, stage_b, x_buf,
                     sems, idx_sems):
    phase, tile = pl.program_id(0), pl.program_id(1)
    col_nodes = table.shape[0] // 2

    @pl.when(tile == 0)
    def _():
        def use(buf, offset):
            def body(n, carry):
                for part in range(2):
                    sub = pl.multiple_of(n * 512 + part * 256, 256)
                    proj = jnp.dot(buf[pl.ds(sub, 256), :], w_hidden[...], preferred_element_type=jnp.float32)
                    proj = proj.astype(jnp.bfloat16).astype(jnp.float32)
                    store_table(table, offset + sub, proj, 2)
                return carry

            lax.fori_loop(0, x_buf.shape[1] // 512, body, 0)

        stream_rows(x_hbm, x_buf, sems, phase, pl.num_programs(0), col_nodes, use)

    forward_step(idx_hbm, w_ref, table, acc, [ids_a, ids_b, ids_c, ids_d], [stage_a, stage_b], idx_sems, 2)

    @pl.when(phase == pl.num_programs(0) - 1)
    def _():
        def use(at, sums):
            z_one = sums.astype(jnp.bfloat16)
            z_ref[at, :] = z_one
            h_one = jnp.maximum(z_one, 0)
            p_ref[at, :] = jnp.dot(h_one, w_output[...], preferred_element_type=jnp.float32).astype(jnp.bfloat16)

        finish_rows(acc, use)


def unpack_table(table, p_hbm, p_buf, sems, phase, phases, blocks, nodes):
    packed = packed_rows(nodes)
    piece = packed // 18

    def use(buf, offset):
        block = offset // packed

        def body(n, carry):
            inside = pl.multiple_of(n * piece, 16)
            value = buf[pl.ds(inside, piece), :].astype(jnp.float32)
            for q in range(PACK):
                turned = value if q == 0 else pltpu.roll(value, LANES - q * pack_lanes(), 1)
                first = pl.multiple_of(block * nodes + q * packed + inside, 16)
                table[pl.ds(first, piece), :] = turned.astype(table.dtype)
            return carry

        lax.fori_loop(0, 18, body, 0)

    stream_rows(p_hbm, p_buf, sems, phase, phases, blocks * packed, use)


def pack_lanes():
    return LANES // PACK // 8 * 8


def packed_rows(nodes):
    return -(-nodes // (PACK * 96)) * 96


def pack_nodes(values):
    nodes = values.shape[0]
    packed = packed_rows(nodes)
    values = jnp.pad(values, ((0, PACK * packed - nodes), (0, pack_lanes() - values.shape[1])))
    parts = [values[q * packed:(q + 1) * packed] for q in range(PACK)]
    return jnp.pad(jnp.concatenate(parts, axis=1), ((0, 0), (0, LANES - PACK * pack_lanes())))


def layer_two_kernel(nodes, idx_hbm, w_ref, p_hbm, z_ref, table, acc, ids_a, ids_b, ids_c, ids_d, stage_a, stage_b, p_buf, sems, idx_sems):
    phase, tile = pl.program_id(0), pl.program_id(1)

    @pl.when(tile == 0)
    def _():
        unpack_table(table, p_hbm, p_buf, sems, phase, pl.num_programs(0), 2, nodes)

    forward_step(idx_hbm, w_ref, table, acc, [ids_a, ids_b, ids_c, ids_d], [stage_a, stage_b], idx_sems, 1)

    @pl.when(phase == pl.num_programs(0) - 1)
    def _():
        def use(at, sums):
            z_ref[at, :] = sums

        finish_rows(acc, use)


def segment_kernel(width, n_src, build, active_ref, over_ref, base_ref, last_ref, idx_hbm, col_ref, w_ref, *refs):
    bufs = STEP_CHUNKS // BUF_CHUNKS
    sources, refs = refs[:n_src], refs[n_src:]
    (out_first, out_second, table, acc, spare_ids, stage_a, stage_b, idx_sems, spare_sem, out_sems), refs = refs[:10], refs[10:]
    ids, refs = refs[:bufs], refs[bufs:]
    buffers, sems = refs[0::2], refs[1::2]
    stages = [stage_a, stage_b]
    phase, tile = pl.program_id(0), pl.program_id(1)
    steps = pl.num_programs(1) * INNER
    total = pl.num_programs(0) * steps

    @pl.when((phase == 0) & (tile == 0))
    def _():
        for buf in range(len(ids)):
            index_copy(idx_hbm, ids, idx_sems, buf, 0).start()

        def zero(n, carry):
            acc[pl.ds(pl.multiple_of(n * 256, 256), 256), :] = jnp.zeros((256, acc.shape[1]), jnp.float32)
            return carry

        lax.fori_loop(0, acc.shape[0] // 256, zero, 0)

    @pl.when(tile == 0)
    def _():
        build(sources, buffers, sems, phase, pl.num_programs(0), table)

    def gathered(stage):
        lanes = []
        for part in range(width):
            rows = stage[pl.ds(part, CHUNK, stride=width), :] if width > 1 else stage[...]
            lanes.append(rows.astype(jnp.bfloat16))
        return jnp.concatenate(lanes, axis=1) if width > 1 else lanes[0]

    def product(cols, weights, rows, base):
        local = lax.broadcasted_iota(jnp.int32, (WINDOW, CHUNK), 0)
        select = jnp.where(local == cols - base, weights, 0.0).astype(jnp.bfloat16)
        acc[pl.ds(pl.multiple_of(base, 8), WINDOW), :] += jnp.dot(select, rows, preferred_element_type=jnp.float32)

    def inner(n, carry):
        place = tile * INNER + n
        step = phase * steps + place
        following = jnp.where(place + 1 < active_ref[phase], step + 1, (phase + 1) * steps)

        def lanes_of(chunk):
            return pl.ds(pl.multiple_of((n * STEP_CHUNKS + chunk) * CHUNK, CHUNK), CHUNK)

        def multiply(chunk):
            part = lanes_of(chunk)
            base = base_ref[step * STEP_CHUNKS + chunk]
            local = lax.broadcasted_iota(jnp.int32, (WINDOW, CHUNK), 0)
            select = jnp.where(local == col_ref[0, :, part] - base, w_ref[0, :, part], 0.0).astype(jnp.bfloat16)
            return base, jnp.dot(select, gathered(stages[chunk % 2]), preferred_element_type=jnp.float32)

        size = WINDOW // PIECES
        for chunk in range(STEP_CHUNKS + 1):
            buf, part = chunk // BUF_CHUNKS, chunk % BUF_CHUNKS
            if part == 0 and chunk < STEP_CHUNKS:
                index_copy(idx_hbm, ids, idx_sems, buf, step).wait()
            if chunk > 0:
                base, sums = multiply(chunk - 1)
            for piece in range(PIECES):
                if chunk < STEP_CHUNKS:
                    for e in range(piece * CHUNK // PIECES, (piece + 1) * CHUNK // PIECES):
                        copy_row(ids[buf], part * CHUNK + e, table, stages[chunk % 2], e, width)
                if chunk > 0:
                    at = pl.ds(pl.multiple_of(base + piece * size, 8), size)
                    acc[at, :] += sums[piece * size:(piece + 1) * size, :]
            if part == BUF_CHUNKS - 1 and chunk < STEP_CHUNKS:
                start_next(idx_hbm, ids, idx_sems, buf, following, total)

        @pl.when(over_ref[step] > 0)
        def _():
            wide_chunks(n, step)

        return carry

    def wide_chunks(n, step):
        size = STEP_CHUNKS * CHUNK
        copy = pltpu.make_async_copy(idx_hbm.at[pl.ds(pl.multiple_of(step * size, size), size)], spare_ids, spare_sem)
        copy.start()
        copy.wait()

        def wide(chunk, carry):
            base, last = base_ref[step * STEP_CHUNKS + chunk], last_ref[step * STEP_CHUNKS + chunk]

            @pl.when(last >= base + WINDOW)
            def _():
                def fetch(e, carry):
                    copy_row(spare_ids, chunk * CHUNK + e, table, stage_a, 0, width)
                    if width == 1:
                        stage_b[pl.ds(e, 1), :] = stage_a[0:1, :]
                    else:
                        stage_b[pl.ds(width * e, width), :] = stage_a[0:width, :]
                    return carry

                lax.fori_loop(0, CHUNK, fetch, 0)
                part = pl.ds(pl.multiple_of((n * STEP_CHUNKS + chunk) * CHUNK, CHUNK), CHUNK)
                cols, weights = col_ref[0, :, part], w_ref[0, :, part]
                rows = gathered(stage_b)
                end = acc.shape[0] - WINDOW

                def more(window, carry):
                    start = base + window * WINDOW
                    fresh = jnp.where(cols >= start, weights, 0.0)
                    product(cols, fresh, rows, jnp.minimum(start, end))
                    return carry

                lax.fori_loop(1, (last - base) // WINDOW + 1, more, 0)

            return carry

        lax.fori_loop(0, STEP_CHUNKS, wide, 0)

    lax.fori_loop(0, jnp.clip(active_ref[phase] - tile * INNER, 0, INNER), inner, 0)

    @pl.when((phase == pl.num_programs(0) - 1) & (tile == pl.num_programs(1) - 1))
    def _():
        half = acc.shape[0] // 2
        copies = [pltpu.make_async_copy(acc.at[pl.ds(n * half, half), :], out, out_sems.at[n])
                  for n, out in enumerate([out_first, out_second])]
        for copy in copies:
            copy.start()
        for copy in copies:
            copy.wait()


def build_packed(nodes, sources, buffers, sems, phase, phases, table):
    unpack_table(table, sources[0], buffers[0], sems[0], phase, phases, 1, nodes)


def build_dz(nodes, sources, buffers, sems, phase, phases, table):
    z_first, z_second, b_hbm, w_out = sources
    z_buf, b_buf, back = buffers
    half = nodes // 2
    unpack_table(back, b_hbm, b_buf, sems[1], phase, phases, 1, nodes)

    def use(buf, offset):
        for sub in range(0, z_buf.shape[2], 256):
            z_one = buf[sub:sub + 256, :]
            back_two = back[pl.ds(pl.multiple_of(offset + sub, 256), 256), :]
            dh_one = lax.dot_general(back_two, w_out[...], CONTRACT_COLS, preferred_element_type=jnp.float32)
            dz_one = jnp.where(z_one.astype(jnp.float32) > 0, dh_one, 0.0).astype(jnp.bfloat16)
            store_table(table, offset + sub, dz_one.astype(jnp.float32), 2)

    stream_rows(z_first, z_buf.at[0], sems[0].at[0], phase, phases, half, use)
    stream_rows(z_second, z_buf.at[1], sems[0].at[1], phase, phases, half, lambda buf, offset: use(buf, half + offset))


def params():
    return pltpu.CompilerParams(vmem_limit_bytes=VMEM, dimension_semantics=("arbitrary", "arbitrary"))


def forward_specs(weights, last):
    slots = weights.shape[1]
    rows = INNER * STEP_SUBS * SUB_ROWS
    w_spec = pl.BlockSpec((1, slots, rows), lambda k, t: (k, 0, t))

    def out_spec(width):
        return pl.BlockSpec((rows, width), lambda k, t: (jnp.where(k == last, t, 0), 0))

    ids = pltpu.SMEM((BUF_SUBS * slots * SUB_ROWS,), jnp.int32)
    return w_spec, out_spec, [ids] * (STEP_SUBS // BUF_SUBS)


def layer_one(idx, weights, x_all, w_hidden, w_out_pad):
    phases, slots, rows = weights.shape
    nodes, feat = x_all.shape
    hid = w_hidden.shape[1]
    whole = pl.BlockSpec(memory_space=pltpu.VMEM)
    any_spec = pl.BlockSpec(memory_space=pl.ANY)
    w_spec, out_spec, ids = forward_specs(weights, phases - 1)
    stage = pltpu.VMEM((2 * slots * SUB_ROWS, LANES), jnp.float32)
    return pl.pallas_call(
        layer_one_kernel,
        grid=(phases, rows // (INNER * STEP_SUBS * SUB_ROWS)),
        in_specs=[any_spec, w_spec, any_spec, whole, whole],
        out_specs=[out_spec(hid), out_spec(LANES)],
        out_shape=[jax.ShapeDtypeStruct((rows, hid), jnp.bfloat16), jax.ShapeDtypeStruct((rows, LANES), jnp.bfloat16)],
        scratch_shapes=[
            pltpu.VMEM((2 * nodes // phases, LANES), jnp.float32), pltpu.VMEM((rows, hid), jnp.float32),
            *ids, stage, stage, pltpu.VMEM((2, 4096, feat), jnp.bfloat16),
            pltpu.SemaphoreType.DMA((2,)), pltpu.SemaphoreType.DMA((STEP_SUBS // BUF_SUBS,))],
        compiler_params=params(),
        cost_estimate=pl.CostEstimate(flops=2 * 10**11, bytes_accessed=10**8, transcendentals=0),
        name="layer_one")(idx, weights, x_all, w_hidden, w_out_pad)


def layer_two(idx, weights, p_all):
    phases, slots, rows = weights.shape
    any_spec = pl.BlockSpec(memory_space=pl.ANY)
    w_spec, out_spec, ids = forward_specs(weights, phases - 1)
    stage = pltpu.VMEM((slots * SUB_ROWS, LANES), jnp.float32)
    return pl.pallas_call(
        functools.partial(layer_two_kernel, rows),
        grid=(phases, rows // (INNER * STEP_SUBS * SUB_ROWS)),
        in_specs=[any_spec, w_spec, any_spec],
        out_specs=out_spec(LANES),
        out_shape=jax.ShapeDtypeStruct((rows, LANES), jnp.float32),
        scratch_shapes=[
            pltpu.VMEM((2 * rows + 128, LANES), jnp.float32), pltpu.VMEM((rows, LANES), jnp.float32),
            *ids, stage, stage, pltpu.VMEM((2, packed_rows(rows), LANES), jnp.bfloat16),
            pltpu.SemaphoreType.DMA((2,)), pltpu.SemaphoreType.DMA((STEP_SUBS // BUF_SUBS,))],
        compiler_params=params(),
        cost_estimate=pl.CostEstimate(flops=2 * 10**11, bytes_accessed=10**8, transcendentals=0),
        name="layer_two")(idx, weights, p_all)


def segment_product(build, plan, sources, specs, buffers, num_out, width, rows):
    idx, cols, weights, scalars = plan
    phases, edges = cols.shape
    per_step = INNER * STEP_CHUNKS * CHUNK
    steps = edges // per_step
    any_spec = pl.BlockSpec(memory_space=pl.ANY)
    tile_spec = pl.BlockSpec((1, 1, per_step), lambda p, t, *_: (p * steps + t, 0, 0))
    ids = pltpu.SMEM((BUF_CHUNKS * CHUNK,), jnp.int32)
    stage = pltpu.VMEM((width * CHUNK, LANES), jnp.float32)
    grid_spec = pltpu.PrefetchScalarGridSpec(
        num_scalar_prefetch=len(scalars),
        grid=(phases, steps),
        in_specs=[any_spec, tile_spec, tile_spec, *specs],
        out_specs=[any_spec, any_spec],
        scratch_shapes=[
            pltpu.VMEM((width * rows + (128 if width == 1 else 0), LANES), jnp.float32),
            pltpu.VMEM((num_out, width * LANES), jnp.float32),
            pltpu.SMEM((STEP_CHUNKS * CHUNK,), jnp.int32), stage, stage,
            pltpu.SemaphoreType.DMA((STEP_CHUNKS // BUF_CHUNKS,)), pltpu.SemaphoreType.DMA, pltpu.SemaphoreType.DMA((2,)),
            *([ids] * (STEP_CHUNKS // BUF_CHUNKS)), *buffers])
    return pl.pallas_call(
        functools.partial(segment_kernel, width, len(sources), functools.partial(build, rows)),
        grid_spec=grid_spec,
        out_shape=[jax.ShapeDtypeStruct((num_out // 2, width * LANES), jnp.float32)] * 2,
        compiler_params=params(),
        cost_estimate=pl.CostEstimate(flops=2 * 10**11, bytes_accessed=10**8, transcendentals=0))(*scalars, (idx * width).reshape(-1), cols.reshape(phases * steps, 1, per_step),
                   weights.reshape(phases * steps, 1, per_step), *sources)


def edge_lists(cols_blk, mask_blk, vals_blk, col_blocks, blk_nodes, turn):
    slots = cols_blk.shape[0]
    col_nodes = 2 * blk_nodes
    row_ids = lax.broadcasted_iota(jnp.int32, (slots, col_blocks, blk_nodes), 2)
    valid = mask_blk.reshape(slots, col_blocks, blk_nodes) > 0
    turned = jnp.bitwise_xor(cols_blk, turn).reshape(slots, col_blocks, blk_nodes)
    keys = jnp.where(valid, turned, col_nodes) * blk_nodes + row_ids
    weights = jnp.where(valid, vals_blk.reshape(slots, col_blocks, blk_nodes).astype(jnp.float32), 0.0)
    keys = keys.transpose(1, 0, 2).reshape(col_blocks, slots * blk_nodes)
    return keys, weights.transpose(1, 0, 2).reshape(col_blocks, slots * blk_nodes)


def make_plan(keys, weights, blk_nodes):
    col_nodes = 2 * blk_nodes
    cols, rows = keys // blk_nodes, keys % blk_nodes
    chunked = cols.reshape(-1, CHUNK)
    base = jnp.minimum(chunked[:, 0] // 8 * 8, col_nodes - WINDOW)
    last = jnp.max(jnp.where(chunked < col_nodes, chunked, -1), axis=1)
    over = jnp.max((last >= base + WINDOW).astype(jnp.int32).reshape(-1, STEP_CHUNKS), axis=1)
    count = jnp.sum((cols < col_nodes).astype(jnp.int32), axis=1)
    active = jnp.maximum((count + STEP_CHUNKS * CHUNK - 1) // (STEP_CHUNKS * CHUNK), 1)
    return rows, cols, weights, (active, over, base, last)


def all_reduce_kernel(row_size, col_size, x_ref, out_ref, held, send_a, recv_a, send_b, recv_b):
    devices = row_size * col_size
    me = lax.axis_index("row") * col_size + lax.axis_index("col")
    size = x_ref.shape[0] // devices

    def place(index):
        return {"row": index // col_size, "col": index % col_size}

    barrier = pltpu.get_barrier_semaphore()
    for d in range(1, devices):
        pl.semaphore_signal(barrier, inc=1, device_id=place((me + d) % devices), device_id_type=pl.DeviceIdType.MESH)
    pl.semaphore_wait(barrier, devices - 1)
    copies = []
    for d in range(1, devices):
        peer = (me + d) % devices
        copies.append(pltpu.make_async_remote_copy(
            src_ref=x_ref.at[pl.ds(pl.multiple_of(peer * size, size), size), :], dst_ref=held.at[d - 1],
            send_sem=send_a.at[d - 1], recv_sem=recv_a.at[d - 1], device_id=place(peer), device_id_type=pl.DeviceIdType.MESH))
    for copy in copies:
        copy.start()
    for copy in copies:
        copy.wait()
    mine = pl.ds(pl.multiple_of(me * size, size), size)
    total = x_ref[mine, :]
    for d in range(1, devices):
        total = total + held[d - 1]
    out_ref[mine, :] = total
    copies = []
    for d in range(1, devices):
        copies.append(pltpu.make_async_remote_copy(
            src_ref=out_ref.at[mine, :], dst_ref=out_ref.at[mine, :], send_sem=send_b.at[d - 1], recv_sem=recv_b.at[d - 1],
            device_id=place((me + d) % devices), device_id_type=pl.DeviceIdType.MESH))
    for copy in copies:
        copy.start()
    for copy in copies:
        copy.wait()


def all_reduce(x, row_size, col_size):
    devices = row_size * col_size
    whole = pl.BlockSpec(memory_space=pltpu.VMEM)
    sems = pltpu.SemaphoreType.DMA((devices - 1,))
    return pl.pallas_call(
        functools.partial(all_reduce_kernel, row_size, col_size),
        in_specs=[whole],
        out_specs=whole,
        out_shape=jax.ShapeDtypeStruct(x.shape, x.dtype),
        scratch_shapes=[pltpu.VMEM((devices - 1, x.shape[0] // devices, x.shape[1]), x.dtype), sems, sems, sems, sems],
        compiler_params=pltpu.CompilerParams(collective_id=0, has_side_effects=True),
        name="all_reduce")(x)


def solution(mesh):
    row_size = mesh.shape["row"]
    col_size = mesh.shape["col"]
    both_axes = ("row", "col")
    swap = [(0, 1), (1, 0)]

    def device_step(feat_blk, w_hidden, w_output, cols_blk, vals_blk, mask_blk, labels_blk, train_blk):
        row_i, col_j = lax.axis_index("row"), lax.axis_index("col")
        blk_nodes = feat_blk.shape[0]
        col_nodes = blk_nodes * row_size
        packed = packed_rows(blk_nodes)
        slots = cols_blk.shape[0]
        classes = w_output.shape[1]
        any_spec = pl.BlockSpec(memory_space=pl.ANY)
        whole = pl.BlockSpec(memory_space=pltpu.VMEM)
        w_out_pad = jnp.pad(w_output, ((0, 0), (0, LANES - classes)))

        x_all = lax.all_gather(feat_blk, both_axes, axis=0, tiled=True)
        masked = vals_blk * mask_blk.astype(jnp.bfloat16)
        own_cols = lax.all_to_all(cols_blk, "col", split_axis=1, concat_axis=0, tiled=True)
        own_w = lax.all_to_all(masked, "col", split_axis=1, concat_axis=0, tiled=True)
        own_w = own_w.astype(jnp.float32).reshape(col_size, slots, blk_nodes)
        own_cols = own_cols.reshape(col_size, slots, -1, STEP_SUBS, SUB_ROWS).transpose(0, 2, 3, 1, 4).reshape(-1)

        keys, edge_w = edge_lists(cols_blk, mask_blk, vals_blk, col_size, blk_nodes, (1 - row_i) * blk_nodes)
        edges = lax.sort((keys, edge_w), dimension=1, num_keys=1, is_stable=False)
        x_all, edges = lax.optimization_barrier((x_all, edges))
        plan = make_plan(*edges, blk_nodes)

        z_one, proj_two = layer_one(own_cols * 2, own_w, x_all, w_hidden, w_out_pad)
        count = jnp.sum(train_blk)
        spare = PACK * pack_lanes()
        lane_ids = lax.broadcasted_iota(jnp.int32, (packed, LANES), 1)
        counts = jnp.where(lane_ids == spare, count // 128, jnp.where(lane_ids == spare + 1, count % 128, 0))
        p_all = lax.all_gather(pack_nodes(proj_two[:, :classes]) + counts.astype(jnp.bfloat16), both_axes, axis=0, tiled=True)
        z_one, p_all = lax.optimization_barrier((z_one, p_all))
        z_first = lax.all_gather(z_one[:blk_nodes // 2], "col", axis=0, tiled=True)
        counts = p_all.reshape(row_size * col_size, packed, LANES)[:, 0, spare:spare + 2].astype(jnp.float32)
        train_count = jnp.maximum(jnp.sum(counts[:, 0] * 128.0 + counts[:, 1]), 1.0)
        z_two = layer_two(own_cols, own_w, p_all)[:, :classes]

        mask_f = train_blk.astype(jnp.float32)
        log_norm = jax.nn.logsumexp(z_two, axis=1)
        onehot = (labels_blk[:, None] == jnp.arange(classes, dtype=jnp.int32)[None, :]).astype(jnp.float32)
        picked = jnp.sum(z_two * onehot, axis=1)
        loss_mean = jnp.sum(mask_f * (log_norm - picked)) / train_count
        softmax_z = jnp.exp(z_two - log_norm[:, None])
        grad_two = ((mask_f / train_count)[:, None] * (softmax_z - onehot)).astype(jnp.bfloat16)
        z_first, grad_two = lax.optimization_barrier((z_first, grad_two))
        grad_rows = lax.all_gather(pack_nodes(grad_two), "col", axis=0, tiled=True)
        z_later, grad_rows = lax.optimization_barrier((z_one[blk_nodes // 2:], grad_rows))
        z_second = lax.all_gather(z_later, "col", axis=0, tiled=True)

        row_bufs = [pltpu.VMEM((1, packed, LANES), jnp.bfloat16), pltpu.SemaphoreType.DMA((1,))]
        send_two, keep_two = segment_product(
            build_packed, plan, [grad_rows], [any_spec], row_bufs, col_nodes, 1, blk_nodes)
        back_two = (keep_two + lax.ppermute(send_two, "row", swap)).astype(jnp.bfloat16)
        z_second, back_two = lax.optimization_barrier((z_second, back_two))
        back_all = lax.all_gather(pack_nodes(back_two[:, :classes]), ("col", "row"), axis=0, tiled=True)
        back_rows = lax.dynamic_slice_in_dim(back_all, row_i * col_size * packed, col_size * packed, 0)
        back_own = lax.dynamic_slice_in_dim(back_rows, col_j * packed, packed, 0)
        back_own = jnp.concatenate([back_own[:, q * pack_lanes():q * pack_lanes() + classes] for q in range(PACK)], axis=0)[:blk_nodes]
        h_one = jnp.maximum(z_one, 0)
        grad_w_output = lax.dot_general(h_one, back_own, CONTRACT_ROWS, preferred_element_type=jnp.float32)

        send_one, keep_one = segment_product(
            build_dz, plan, [z_first, z_second, back_rows, w_out_pad], [any_spec, any_spec, any_spec, whole],
            [pltpu.VMEM((2, 4, 1024, 2 * LANES), jnp.bfloat16), pltpu.SemaphoreType.DMA((2, 4)), *row_bufs,
             pltpu.VMEM((blk_nodes + 128, LANES), jnp.bfloat16)],
            col_nodes, 2, blk_nodes)
        back_one = (keep_one + lax.ppermute(send_one, "row", swap)).astype(jnp.bfloat16)
        feat_src = lax.dynamic_slice_in_dim(x_all, (col_j * row_size + row_i) * blk_nodes, blk_nodes, 0)
        grad_w_hidden = lax.dot_general(feat_src, back_one, CONTRACT_ROWS, preferred_element_type=jnp.float32)
        feat, hid = w_hidden.shape
        out_pad = jnp.pad(grad_w_output, ((0, 0), (0, LANES - classes)))
        rows = feat * hid // LANES + hid
        packed_out = jnp.concatenate([grad_w_hidden.reshape(-1, LANES), out_pad, jnp.full((1, LANES), loss_mean)], axis=0)
        unit = 8 * row_size * col_size
        packed_out = jnp.pad(packed_out, ((0, -(rows + 1) % unit), (0, 0)))
        total = all_reduce(packed_out, row_size, col_size)
        grad_w_hidden = total[:feat * hid // LANES].reshape(feat, hid)
        return total[rows, 0], grad_w_hidden, total[feat * hid // LANES:rows, :classes]

    node_spec = P(("row", "col"), None)
    label_spec = P(("row", "col"))
    adj_spec = P("col", "row")
    return jax.shard_map(device_step, mesh=mesh, in_specs=(node_spec, P(), P(), adj_spec, adj_spec, adj_spec, label_spec, label_spec), out_specs=(P(), P(), P()), check_vma=False)
```

```python
import functools

import jax
import jax.numpy as jnp
from jax import lax
from jax.experimental import pallas as pl
from jax.experimental.pallas import tpu as pltpu
from jax.sharding import PartitionSpec as P


CONTRACT_ROWS = (((0,), (0,)), ((), ()))
CONTRACT_COLS = (((1,), (1,)), ((), ()))
LANES = 128
SUB_ROWS = 256
STEP_SUBS = 4
PIECE_ROWS = 32
PIECES = 8
BUF_SUBS = 1
CHUNK = 256
BUF_CHUNKS = 2
STEP_CHUNKS = 16
WINDOW = 256
PACK = 3
INNER = 4
VMEM = 63 << 20


def copy_row(ids, e, table, stage, at, width):
    if width == 1:
        stage[at, :] = table[ids[e], :]
    else:
        stage[width * at:width * (at + 1), :] = table[pl.ds(pl.multiple_of(ids[e], width), width), :]


def index_copy(idx_hbm, ids, sems, buf, step):
    size = ids[buf].shape[0]
    start = pl.multiple_of((step * len(ids) + buf) * size, size)
    return pltpu.make_async_copy(idx_hbm.at[pl.ds(start, size)], ids[buf], sems.at[buf])


def start_next(idx_hbm, ids, sems, buf, following, total):
    @pl.when(following < total)
    def _():
        index_copy(idx_hbm, ids, sems, buf, following).start()


def store_table(table, first, value, width):
    rows = value.shape[0]
    for part in range(width):
        piece = value[:, part * LANES:(part + 1) * LANES]
        if width == 1:
            table[pl.ds(pl.multiple_of(first, rows), rows), :] = piece
        else:
            table[pl.ds(width * first + part, rows, stride=width), :] = piece


def stream_rows(source, buffer, sems, phase, phases, total, use):
    slots, chunk = buffer.shape[0], buffer.shape[1]
    steps = total // chunk
    assert steps % slots == 0

    def copy(step, slot):
        start = pl.multiple_of(phase * total + step * chunk, 16)
        return pltpu.make_async_copy(source.at[pl.ds(start, chunk), :], buffer.at[slot], sems.at[slot])

    @pl.when(phase == 0)
    def _():
        for slot in range(slots):
            copy(slot, slot).start()

    def body(group, carry):
        for slot in range(slots):
            step = group * slots + slot
            copy(step, slot).wait()
            use(buffer.at[slot], step * chunk)

            @pl.when((step + slots < steps) | (phase + 1 < phases))
            def _():
                copy(step + slots, slot).start()
        return carry

    lax.fori_loop(0, steps // slots, body, 0)


def weight_columns(w_ref, first):
    w_rows = w_ref[0, :, pl.ds(pl.multiple_of(first, LANES), LANES)]
    return jnp.concatenate([w_rows] * (8 // w_ref.shape[1]), axis=0).T


def weighted_sum(stage, w_cols, slots, first, size, width):
    parts = [None] * width
    inside = first % LANES
    for slot in range(slots):
        column = jnp.broadcast_to(w_cols[inside:inside + size, slot:slot + 1], (size, LANES))
        at = width * (slot * SUB_ROWS + first)
        for part in range(width):
            rows = stage[pl.ds(at + part, size, stride=width), :] if width > 1 else stage[at:at + size, :]
            term = column * rows
            parts[part] = term if slot == 0 else parts[part] + term
    return parts


def forward_step(idx_hbm, w_ref, table, acc, ids, stages, idx_sems, width):
    phase, tile = pl.program_id(0), pl.program_id(1)
    per_phase = pl.num_programs(1) * INNER
    total = pl.num_programs(0) * per_phase
    slots = w_ref.shape[1]
    edges = slots * SUB_ROWS
    pieces = SUB_ROWS // PIECE_ROWS
    step_rows = STEP_SUBS * SUB_ROWS

    @pl.when((phase == 0) & (tile == 0))
    def _():
        for buf in range(len(ids)):
            index_copy(idx_hbm, ids, idx_sems, buf, 0).start()

    def inner(n, carry):
        step = phase * per_phase + tile * INNER + n
        first_row = pl.multiple_of((tile * INNER + n) * step_rows, step_rows)

        @pl.when(phase == 0)
        def _():
            acc[pl.ds(first_row, step_rows), :] = jnp.zeros((step_rows, acc.shape[1]), jnp.float32)

        for sub in range(STEP_SUBS + 1):
            buf, part = sub // BUF_SUBS, sub % BUF_SUBS
            if part == 0 and sub < STEP_SUBS:
                index_copy(idx_hbm, ids, idx_sems, buf, step).wait()
            for piece in range(pieces):
                first = piece * PIECE_ROWS
                if sub > 0 and first % LANES == 0:
                    w_cols = weight_columns(w_ref, n * step_rows + (sub - 1) * SUB_ROWS + first)
                if sub < STEP_SUBS:
                    for e in range(piece * edges // pieces, (piece + 1) * edges // pieces):
                        copy_row(ids[buf], part * edges + e, table, stages[sub % len(stages)], e, width)
                if sub > 0:
                    parts = weighted_sum(stages[(sub - 1) % len(stages)], w_cols, slots, first, PIECE_ROWS, width)
                    rows = pl.ds(pl.multiple_of(first_row + (sub - 1) * SUB_ROWS + first, PIECE_ROWS), PIECE_ROWS)
                    for lane in range(width):
                        acc[rows, lane * LANES:(lane + 1) * LANES] += parts[lane]
            if part == BUF_SUBS - 1 and sub < STEP_SUBS:
                start_next(idx_hbm, ids, idx_sems, buf, step + 1, total)
        return carry

    lax.fori_loop(0, INNER, inner, 0)


def finish_rows(acc, use):
    tile = pl.program_id(1)
    size = INNER * STEP_SUBS * SUB_ROWS

    def body(n, carry):
        at = pl.multiple_of(n * 256, 256)
        use(pl.ds(at, 256), acc[pl.ds(pl.multiple_of(tile * size + at, 256), 256), :])
        return carry

    lax.fori_loop(0, size // 256, body, 0)


def layer_one_kernel(idx_hbm, w_ref, x_hbm, w_hidden, w_output, z_ref, p_ref, table, acc, ids_a, ids_b, ids_c, ids_d, stage_a, stage_b, x_buf,
                     sems, idx_sems):
    phase, tile = pl.program_id(0), pl.program_id(1)
    col_nodes = table.shape[0] // 2

    @pl.when(tile == 0)
    def _():
        def use(buf, offset):
            def body(n, carry):
                for part in range(2):
                    sub = pl.multiple_of(n * 512 + part * 256, 256)
                    proj = jnp.dot(buf[pl.ds(sub, 256), :], w_hidden[...], preferred_element_type=jnp.float32)
                    proj = proj.astype(jnp.bfloat16).astype(jnp.float32)
                    store_table(table, offset + sub, proj, 2)
                return carry

            lax.fori_loop(0, x_buf.shape[1] // 512, body, 0)

        stream_rows(x_hbm, x_buf, sems, phase, pl.num_programs(0), col_nodes, use)

    forward_step(idx_hbm, w_ref, table, acc, [ids_a, ids_b, ids_c, ids_d], [stage_a, stage_b], idx_sems, 2)

    @pl.when(phase == pl.num_programs(0) - 1)
    def _():
        def use(at, sums):
            z_one = sums.astype(jnp.bfloat16)
            z_ref[at, :] = z_one
            h_one = jnp.maximum(z_one, 0)
            p_ref[at, :] = jnp.dot(h_one, w_output[...], preferred_element_type=jnp.float32).astype(jnp.bfloat16)

        finish_rows(acc, use)


def unpack_table(table, p_hbm, p_buf, sems, phase, phases, blocks, nodes):
    packed = packed_rows(nodes)
    piece = packed // 18

    def use(buf, offset):
        block = offset // packed

        def body(n, carry):
            inside = pl.multiple_of(n * piece, 16)
            value = buf[pl.ds(inside, piece), :].astype(jnp.float32)
            for q in range(PACK):
                turned = value if q == 0 else pltpu.roll(value, LANES - q * pack_lanes(), 1)
                first = pl.multiple_of(block * nodes + q * packed + inside, 16)
                table[pl.ds(first, piece), :] = turned.astype(table.dtype)
            return carry

        lax.fori_loop(0, 18, body, 0)

    stream_rows(p_hbm, p_buf, sems, phase, phases, blocks * packed, use)


def pack_lanes():
    return LANES // PACK // 8 * 8


def packed_rows(nodes):
    return -(-nodes // (PACK * 96)) * 96


def pack_nodes(values):
    nodes = values.shape[0]
    packed = packed_rows(nodes)
    values = jnp.pad(values, ((0, PACK * packed - nodes), (0, pack_lanes() - values.shape[1])))
    parts = [values[q * packed:(q + 1) * packed] for q in range(PACK)]
    return jnp.pad(jnp.concatenate(parts, axis=1), ((0, 0), (0, LANES - PACK * pack_lanes())))


def pack_rows(acc, first, piece, packed, n):
    lane = lax.broadcasted_iota(jnp.int32, (piece, LANES), 1)
    total = None
    for q in range(PACK):
        rows = acc[pl.ds(pl.multiple_of(first + q * packed + n * piece, 8), piece), :]
        rows = jnp.where(lane < pack_lanes(), rows, 0.0)
        rows = rows if q == 0 else pltpu.roll(rows, q * pack_lanes(), 1)
        total = rows if q == 0 else total + rows
    return total


def layer_two_kernel(nodes, classes, idx_hbm, w_ref, p_hbm, node_ref, count_ref, grad_ref, loss_ref, table, acc, ids_a, ids_b,
                     ids_c, ids_d, stage_a, stage_b, p_buf, sems, idx_sems):
    phase, tile = pl.program_id(0), pl.program_id(1)
    packed = packed_rows(nodes)

    @pl.when((phase == 0) & (tile == 0))
    def _():
        acc[nodes:, :] = jnp.zeros((acc.shape[0] - nodes, LANES), jnp.float32)
        loss_ref[...] = jnp.zeros_like(loss_ref)

    @pl.when(tile == 0)
    def _():
        unpack_table(table, p_hbm, p_buf, sems, phase, pl.num_programs(0), 2, nodes)

    forward_step(idx_hbm, w_ref, table, acc, [ids_a, ids_b, ids_c, ids_d], [stage_a, stage_b], idx_sems, 1)

    @pl.when(phase == pl.num_programs(0) - 1)
    def _():
        size = INNER * STEP_SUBS * SUB_ROWS
        group = 512
        lane = lax.broadcasted_iota(jnp.int32, (group, LANES), 1)
        lane_f = lane.astype(jnp.float32)
        count = count_ref[0]

        def body(n, carry):
            rows = pl.ds(pl.multiple_of(tile * size + n * group, group), group)
            columns = node_ref[:, rows].T
            label = jnp.broadcast_to(columns[:, 0:1], (group, LANES))
            mask = jnp.broadcast_to(columns[:, 1:2], (group, LANES))
            z_two = jnp.where(lane < classes, acc[rows, :], -jnp.inf)
            top = jnp.max(z_two, axis=1, keepdims=True)
            log_norm = jnp.log(jnp.sum(jnp.exp(z_two - top), axis=1, keepdims=True)) + top
            hit = lane_f == label
            terms = mask * (jnp.where(lane == 0, log_norm, 0.0) - jnp.where(hit, z_two, 0.0))
            loss_ref[...] += jnp.sum(terms.reshape(group // 8, 8, LANES), axis=0)
            acc[rows, :] = (mask / count) * (jnp.exp(z_two - log_norm) - jnp.where(hit, 1.0, 0.0))
            return carry

        lax.fori_loop(0, size // group, body, 0)

    @pl.when((phase == pl.num_programs(0) - 1) & (tile == pl.num_programs(1) - 1))
    def _():
        piece = packed // 18

        def body(n, carry):
            grad_ref[pl.ds(pl.multiple_of(n * piece, 16), piece), :] = pack_rows(acc, 0, piece, packed, n).astype(jnp.bfloat16)
            return carry

        lax.fori_loop(0, 18, body, 0)


def segment_kernel(width, nodes, n_src, build, active_ref, over_ref, base_ref, last_ref, idx_hbm, col_ref, w_ref, *refs):
    bufs = STEP_CHUNKS // BUF_CHUNKS
    sources, refs = refs[:n_src], refs[n_src:]
    (out_first, out_second, table, acc, spare_ids, stage_a, stage_b, idx_sems, spare_sem, out_sems), refs = refs[:10], refs[10:]
    ids, refs = refs[:bufs], refs[bufs:]
    if width == 1:
        packed_sums, refs = refs[0], refs[1:]
    buffers, sems = refs[0::2], refs[1::2]
    stages = [stage_a, stage_b]
    phase, tile = pl.program_id(0), pl.program_id(1)
    steps = pl.num_programs(1) * INNER
    total = pl.num_programs(0) * steps

    @pl.when((phase == 0) & (tile == 0))
    def _():
        for buf in range(len(ids)):
            index_copy(idx_hbm, ids, idx_sems, buf, 0).start()

        def zero(n, carry):
            acc[pl.ds(pl.multiple_of(n * 256, 256), 256), :] = jnp.zeros((256, acc.shape[1]), jnp.float32)
            return carry

        lax.fori_loop(0, acc.shape[0] // 256, zero, 0)

    @pl.when(tile == 0)
    def _():
        build(sources, buffers, sems, phase, pl.num_programs(0), table)

    def gathered(stage):
        lanes = []
        for part in range(width):
            rows = stage[pl.ds(part, CHUNK, stride=width), :] if width > 1 else stage[...]
            lanes.append(rows.astype(jnp.bfloat16))
        return jnp.concatenate(lanes, axis=1) if width > 1 else lanes[0]

    def product(cols, weights, rows, base):
        local = lax.broadcasted_iota(jnp.int32, (WINDOW, CHUNK), 0)
        select = jnp.where(local == cols - base, weights, 0.0).astype(jnp.bfloat16)
        acc[pl.ds(pl.multiple_of(base, 8), WINDOW), :] += jnp.dot(select, rows, preferred_element_type=jnp.float32)

    def inner(n, carry):
        place = tile * INNER + n
        step = phase * steps + place
        following = jnp.where(place + 1 < active_ref[phase], step + 1, (phase + 1) * steps)

        def lanes_of(chunk):
            return pl.ds(pl.multiple_of((n * STEP_CHUNKS + chunk) * CHUNK, CHUNK), CHUNK)

        def multiply(chunk):
            part = lanes_of(chunk)
            base = base_ref[step * STEP_CHUNKS + chunk]
            local = lax.broadcasted_iota(jnp.int32, (WINDOW, CHUNK), 0)
            select = jnp.where(local == col_ref[0, :, part] - base, w_ref[0, :, part], 0.0).astype(jnp.bfloat16)
            return base, jnp.dot(select, gathered(stages[chunk % 2]), preferred_element_type=jnp.float32)

        size = WINDOW // PIECES
        for chunk in range(STEP_CHUNKS + 1):
            buf, part = chunk // BUF_CHUNKS, chunk % BUF_CHUNKS
            if part == 0 and chunk < STEP_CHUNKS:
                index_copy(idx_hbm, ids, idx_sems, buf, step).wait()
            if chunk > 0:
                base, sums = multiply(chunk - 1)
            for piece in range(PIECES):
                if chunk < STEP_CHUNKS:
                    for e in range(piece * CHUNK // PIECES, (piece + 1) * CHUNK // PIECES):
                        copy_row(ids[buf], part * CHUNK + e, table, stages[chunk % 2], e, width)
                if chunk > 0:
                    at = pl.ds(pl.multiple_of(base + piece * size, 8), size)
                    acc[at, :] += sums[piece * size:(piece + 1) * size, :]
            if part == BUF_CHUNKS - 1 and chunk < STEP_CHUNKS:
                start_next(idx_hbm, ids, idx_sems, buf, following, total)

        @pl.when(over_ref[step] > 0)
        def _():
            wide_chunks(n, step)

        return carry

    def wide_chunks(n, step):
        size = STEP_CHUNKS * CHUNK
        copy = pltpu.make_async_copy(idx_hbm.at[pl.ds(pl.multiple_of(step * size, size), size)], spare_ids, spare_sem)
        copy.start()
        copy.wait()

        def wide(chunk, carry):
            base, last = base_ref[step * STEP_CHUNKS + chunk], last_ref[step * STEP_CHUNKS + chunk]

            @pl.when(last >= base + WINDOW)
            def _():
                def fetch(e, carry):
                    copy_row(spare_ids, chunk * CHUNK + e, table, stage_a, 0, width)
                    if width == 1:
                        stage_b[pl.ds(e, 1), :] = stage_a[0:1, :]
                    else:
                        stage_b[pl.ds(width * e, width), :] = stage_a[0:width, :]
                    return carry

                lax.fori_loop(0, CHUNK, fetch, 0)
                part = pl.ds(pl.multiple_of((n * STEP_CHUNKS + chunk) * CHUNK, CHUNK), CHUNK)
                cols, weights = col_ref[0, :, part], w_ref[0, :, part]
                rows = gathered(stage_b)
                end = acc.shape[0] - WINDOW

                def more(window, carry):
                    start = base + window * WINDOW
                    fresh = jnp.where(cols >= start, weights, 0.0)
                    product(cols, fresh, rows, jnp.minimum(start, end))
                    return carry

                lax.fori_loop(1, (last - base) // WINDOW + 1, more, 0)

            return carry

        lax.fori_loop(0, STEP_CHUNKS, wide, 0)

    lax.fori_loop(0, jnp.clip(active_ref[phase] - tile * INNER, 0, INNER), inner, 0)

    @pl.when((phase == pl.num_programs(0) - 1) & (tile == pl.num_programs(1) - 1))
    def _():
        half = nodes
        if width == 1:
            packed = packed_rows(nodes)
            piece = packed // 18
            for part in range(2):
                def body(n, carry):
                    at = pl.ds(pl.multiple_of(n * piece, 8), piece)
                    packed_sums[part, at, :] = pack_rows(acc, part * half, piece, packed, n)
                    return carry

                lax.fori_loop(0, 18, body, 0)
            results = [packed_sums.at[0], packed_sums.at[1]]
        else:
            results = [acc.at[pl.ds(part * half, half), :] for part in range(2)]
        copies = [pltpu.make_async_copy(result, out, out_sems.at[n])
                  for n, (result, out) in enumerate(zip(results, [out_first, out_second]))]
        for copy in copies:
            copy.start()
        for copy in copies:
            copy.wait()


def build_packed(nodes, sources, buffers, sems, phase, phases, table):
    unpack_table(table, sources[0], buffers[0], sems[0], phase, phases, 1, nodes)


def build_dz(nodes, sources, buffers, sems, phase, phases, table):
    z_first, z_second, b_hbm, w_out = sources
    z_buf, b_buf, back = buffers
    half = nodes // 2
    unpack_table(back, b_hbm, b_buf, sems[1], phase, phases, 1, nodes)

    def use(buf, offset):
        for sub in range(0, z_buf.shape[2], 256):
            z_one = buf[sub:sub + 256, :]
            back_two = back[pl.ds(pl.multiple_of(offset + sub, 256), 256), :]
            dh_one = lax.dot_general(back_two, w_out[...], CONTRACT_COLS, preferred_element_type=jnp.float32)
            dz_one = jnp.where(z_one.astype(jnp.float32) > 0, dh_one, 0.0).astype(jnp.bfloat16)
            store_table(table, offset + sub, dz_one.astype(jnp.float32), 2)

    stream_rows(z_first, z_buf.at[0], sems[0].at[0], phase, phases, half, use)
    stream_rows(z_second, z_buf.at[1], sems[0].at[1], phase, phases, half, lambda buf, offset: use(buf, half + offset))


def params():
    return pltpu.CompilerParams(vmem_limit_bytes=VMEM, dimension_semantics=("arbitrary", "arbitrary"))


def forward_specs(weights, last):
    slots = weights.shape[1]
    rows = INNER * STEP_SUBS * SUB_ROWS
    w_spec = pl.BlockSpec((1, slots, rows), lambda k, t: (k, 0, t))

    def out_spec(width):
        return pl.BlockSpec((rows, width), lambda k, t: (jnp.where(k == last, t, 0), 0))

    ids = pltpu.SMEM((BUF_SUBS * slots * SUB_ROWS,), jnp.int32)
    return w_spec, out_spec, [ids] * (STEP_SUBS // BUF_SUBS)


def layer_one(idx, weights, x_all, w_hidden, w_out_pad):
    phases, slots, rows = weights.shape
    nodes, feat = x_all.shape
    hid = w_hidden.shape[1]
    whole = pl.BlockSpec(memory_space=pltpu.VMEM)
    any_spec = pl.BlockSpec(memory_space=pl.ANY)
    w_spec, out_spec, ids = forward_specs(weights, phases - 1)
    stage = pltpu.VMEM((2 * slots * SUB_ROWS, LANES), jnp.float32)
    return pl.pallas_call(
        layer_one_kernel,
        grid=(phases, rows // (INNER * STEP_SUBS * SUB_ROWS)),
        in_specs=[any_spec, w_spec, any_spec, whole, whole],
        out_specs=[out_spec(hid), out_spec(LANES)],
        out_shape=[jax.ShapeDtypeStruct((rows, hid), jnp.bfloat16), jax.ShapeDtypeStruct((rows, LANES), jnp.bfloat16)],
        scratch_shapes=[
            pltpu.VMEM((2 * nodes // phases, LANES), jnp.float32), pltpu.VMEM((rows, hid), jnp.float32),
            *ids, stage, stage, pltpu.VMEM((2, 4096, feat), jnp.bfloat16),
            pltpu.SemaphoreType.DMA((2,)), pltpu.SemaphoreType.DMA((STEP_SUBS // BUF_SUBS,))],
        compiler_params=params(),
        cost_estimate=pl.CostEstimate(flops=2 * 10**11, bytes_accessed=10**8, transcendentals=0),
        name="layer_one")(idx, weights, x_all, w_hidden, w_out_pad)


def layer_two(idx, weights, p_all, node_rows, count, classes):
    phases, slots, rows = weights.shape
    any_spec = pl.BlockSpec(memory_space=pl.ANY)
    whole = pl.BlockSpec(memory_space=pltpu.VMEM)
    w_spec, _, ids = forward_specs(weights, phases - 1)
    stage = pltpu.VMEM((slots * SUB_ROWS, LANES), jnp.float32)
    return pl.pallas_call(
        functools.partial(layer_two_kernel, rows, classes),
        grid=(phases, rows // (INNER * STEP_SUBS * SUB_ROWS)),
        in_specs=[any_spec, w_spec, any_spec, whole, pl.BlockSpec(memory_space=pltpu.SMEM)],
        out_specs=[whole, whole],
        out_shape=[jax.ShapeDtypeStruct((packed_rows(rows), LANES), jnp.bfloat16), jax.ShapeDtypeStruct((8, LANES), jnp.float32)],
        scratch_shapes=[
            pltpu.VMEM((2 * rows + 128, LANES), jnp.float32), pltpu.VMEM((rows + 128, LANES), jnp.float32),
            *ids, stage, stage, pltpu.VMEM((2, packed_rows(rows), LANES), jnp.bfloat16),
            pltpu.SemaphoreType.DMA((2,)), pltpu.SemaphoreType.DMA((STEP_SUBS // BUF_SUBS,))],
        compiler_params=params(),
        cost_estimate=pl.CostEstimate(flops=2 * 10**11, bytes_accessed=10**8, transcendentals=0),
        name="layer_two")(idx, weights, p_all, node_rows, count)


def segment_product(build, plan, sources, specs, buffers, num_out, width, rows):
    ids_by_width, cols, weights, scalars = plan
    phases = scalars[0].shape[0]
    steps, per_step = cols.shape[0] // phases, cols.shape[2]
    any_spec = pl.BlockSpec(memory_space=pl.ANY)
    tile_spec = pl.BlockSpec((1, 1, per_step), lambda p, t, *_: (p * steps + t, 0, 0))
    ids = pltpu.SMEM((BUF_CHUNKS * CHUNK,), jnp.int32)
    stage = pltpu.VMEM((width * CHUNK, LANES), jnp.float32)
    out_rows = packed_rows(rows) if width == 1 else num_out // 2
    sums = [pltpu.VMEM((2, out_rows, LANES), jnp.float32)] if width == 1 else []
    grid_spec = pltpu.PrefetchScalarGridSpec(
        num_scalar_prefetch=len(scalars),
        grid=(phases, steps),
        in_specs=[any_spec, tile_spec, tile_spec, *specs],
        out_specs=[any_spec, any_spec],
        scratch_shapes=[
            pltpu.VMEM((width * rows + (128 if width == 1 else 0), LANES), jnp.float32),
            pltpu.VMEM((num_out + (256 if width == 1 else 0), width * LANES), jnp.float32),
            pltpu.SMEM((STEP_CHUNKS * CHUNK,), jnp.int32), stage, stage,
            pltpu.SemaphoreType.DMA((STEP_CHUNKS // BUF_CHUNKS,)), pltpu.SemaphoreType.DMA, pltpu.SemaphoreType.DMA((2,)),
            *([ids] * (STEP_CHUNKS // BUF_CHUNKS)), *sums, *buffers])
    return pl.pallas_call(
        functools.partial(segment_kernel, width, rows, len(sources), functools.partial(build, rows)),
        grid_spec=grid_spec,
        out_shape=[jax.ShapeDtypeStruct((out_rows, width * LANES), jnp.float32)] * 2,
        compiler_params=params(),
        cost_estimate=pl.CostEstimate(flops=2 * 10**11, bytes_accessed=10**8, transcendentals=0))(*scalars, ids_by_width[width - 1], cols, weights, *sources)


def edge_lists(cols_blk, mask_blk, vals_blk, col_blocks, blk_nodes, turn):
    slots = cols_blk.shape[0]
    col_nodes = 2 * blk_nodes
    row_ids = lax.broadcasted_iota(jnp.int32, (slots, col_blocks, blk_nodes), 2)
    valid = mask_blk.reshape(slots, col_blocks, blk_nodes) > 0
    turned = jnp.bitwise_xor(cols_blk, turn).reshape(slots, col_blocks, blk_nodes)
    keys = jnp.where(valid, turned, col_nodes) * blk_nodes + row_ids
    weights = jnp.where(valid, vals_blk.reshape(slots, col_blocks, blk_nodes).astype(jnp.float32), 0.0)
    keys = keys.transpose(1, 0, 2).reshape(col_blocks, slots * blk_nodes)
    return keys, weights.transpose(1, 0, 2).reshape(col_blocks, slots * blk_nodes)


def make_plan(keys, weights, blk_nodes):
    col_nodes = 2 * blk_nodes
    cols, rows = keys // blk_nodes, keys % blk_nodes
    chunked = cols.reshape(-1, CHUNK)
    base = jnp.minimum(chunked[:, 0] // 8 * 8, col_nodes - WINDOW)
    last = jnp.max(jnp.where(chunked < col_nodes, chunked, -1), axis=1)
    over = jnp.max((last >= base + WINDOW).astype(jnp.int32).reshape(-1, STEP_CHUNKS), axis=1)
    count = jnp.sum((cols < col_nodes).astype(jnp.int32), axis=1)
    active = jnp.maximum((count + STEP_CHUNKS * CHUNK - 1) // (STEP_CHUNKS * CHUNK), 1)
    tiles = (-1, 1, INNER * STEP_CHUNKS * CHUNK)
    ids_by_width = (rows.reshape(-1), 2 * rows.reshape(-1))
    return ids_by_width, cols.reshape(tiles), weights.reshape(tiles), (active, over, base, last)


def all_reduce_kernel(row_size, col_size, x_ref, out_ref, held, send_a, recv_a, send_b, recv_b):
    devices = row_size * col_size
    me = lax.axis_index("row") * col_size + lax.axis_index("col")
    size = x_ref.shape[0] // devices

    def place(index):
        return {"row": index // col_size, "col": index % col_size}

    barrier = pltpu.get_barrier_semaphore()
    for d in range(1, devices):
        pl.semaphore_signal(barrier, inc=1, device_id=place((me + d) % devices), device_id_type=pl.DeviceIdType.MESH)
    pl.semaphore_wait(barrier, devices - 1)
    copies = []
    for d in range(1, devices):
        peer = (me + d) % devices
        copies.append(pltpu.make_async_remote_copy(
            src_ref=x_ref.at[pl.ds(pl.multiple_of(peer * size, size), size), :], dst_ref=held.at[d - 1],
            send_sem=send_a.at[d - 1], recv_sem=recv_a.at[d - 1], device_id=place(peer), device_id_type=pl.DeviceIdType.MESH))
    for copy in copies:
        copy.start()
    for copy in copies:
        copy.wait()
    mine = pl.ds(pl.multiple_of(me * size, size), size)
    total = x_ref[mine, :]
    for d in range(1, devices):
        total = total + held[d - 1]
    out_ref[mine, :] = total
    copies = []
    for d in range(1, devices):
        copies.append(pltpu.make_async_remote_copy(
            src_ref=out_ref.at[mine, :], dst_ref=out_ref.at[mine, :], send_sem=send_b.at[d - 1], recv_sem=recv_b.at[d - 1],
            device_id=place((me + d) % devices), device_id_type=pl.DeviceIdType.MESH))
    for copy in copies:
        copy.start()
    for copy in copies:
        copy.wait()


def all_reduce(x, row_size, col_size):
    devices = row_size * col_size
    whole = pl.BlockSpec(memory_space=pltpu.VMEM)
    sems = pltpu.SemaphoreType.DMA((devices - 1,))
    return pl.pallas_call(
        functools.partial(all_reduce_kernel, row_size, col_size),
        in_specs=[whole],
        out_specs=whole,
        out_shape=jax.ShapeDtypeStruct(x.shape, x.dtype),
        scratch_shapes=[pltpu.VMEM((devices - 1, x.shape[0] // devices, x.shape[1]), x.dtype), sems, sems, sems, sems],
        compiler_params=pltpu.CompilerParams(collective_id=0, has_side_effects=True),
        name="all_reduce")(x)


def solution(mesh):
    row_size = mesh.shape["row"]
    col_size = mesh.shape["col"]
    both_axes = ("row", "col")
    swap = [(0, 1), (1, 0)]

    def device_step(feat_blk, w_hidden, w_output, cols_blk, vals_blk, mask_blk, labels_blk, train_blk):
        row_i, col_j = lax.axis_index("row"), lax.axis_index("col")
        blk_nodes = feat_blk.shape[0]
        col_nodes = blk_nodes * row_size
        packed = packed_rows(blk_nodes)
        slots = cols_blk.shape[0]
        classes = w_output.shape[1]
        any_spec = pl.BlockSpec(memory_space=pl.ANY)
        whole = pl.BlockSpec(memory_space=pltpu.VMEM)
        w_out_pad = jnp.pad(w_output, ((0, 0), (0, LANES - classes)))

        x_all = lax.all_gather(feat_blk, both_axes, axis=0, tiled=True)
        masked = vals_blk * mask_blk.astype(jnp.bfloat16)
        own_cols = lax.all_to_all(cols_blk, "col", split_axis=1, concat_axis=0, tiled=True)
        own_w = lax.all_to_all(masked, "col", split_axis=1, concat_axis=0, tiled=True)
        own_w = own_w.astype(jnp.float32).reshape(col_size, slots, blk_nodes)
        own_cols = own_cols.reshape(col_size, slots, -1, STEP_SUBS, SUB_ROWS).transpose(0, 2, 3, 1, 4).reshape(-1)

        keys, edge_w = edge_lists(cols_blk, mask_blk, vals_blk, col_size, blk_nodes, (1 - row_i) * blk_nodes)
        edges = lax.sort((keys, edge_w), dimension=1, num_keys=1, is_stable=False)
        x_all, edges = lax.optimization_barrier((x_all, edges))
        plan = make_plan(*edges, blk_nodes)

        z_one, proj_two = layer_one(own_cols * 2, own_w, x_all, w_hidden, w_out_pad)
        count = jnp.sum(train_blk)
        spare = PACK * pack_lanes()
        lane_ids = lax.broadcasted_iota(jnp.int32, (packed, LANES), 1)
        counts = jnp.where(lane_ids == spare, count // 128, jnp.where(lane_ids == spare + 1, count % 128, 0))
        p_all = lax.all_gather(pack_nodes(proj_two[:, :classes]) + counts.astype(jnp.bfloat16), both_axes, axis=0, tiled=True)
        z_one, p_all, plan = lax.optimization_barrier((z_one, p_all, plan))
        z_first = lax.all_gather(z_one[:blk_nodes // 2], "col", axis=0, tiled=True)
        counts = p_all.reshape(row_size * col_size, packed, LANES)[:, 0, spare:spare + 2].astype(jnp.float32)
        train_count = jnp.maximum(jnp.sum(counts[:, 0] * 128.0 + counts[:, 1]), 1.0)
        node_rows = jnp.zeros((8, blk_nodes), jnp.float32)
        node_rows = node_rows.at[0].set(labels_blk.astype(jnp.float32)).at[1].set(train_blk.astype(jnp.float32))
        grad_two, loss = layer_two(own_cols, own_w, p_all, node_rows, train_count.reshape(1), classes)
        loss_mean = jnp.sum(loss) / train_count
        z_first, grad_two = lax.optimization_barrier((z_first, grad_two))
        grad_rows = lax.all_gather(grad_two, "col", axis=0, tiled=True)
        z_later, grad_rows = lax.optimization_barrier((z_one[blk_nodes // 2:], grad_rows))
        z_second = lax.all_gather(z_later, "col", axis=0, tiled=True)

        row_bufs = [pltpu.VMEM((1, packed, LANES), jnp.bfloat16), pltpu.SemaphoreType.DMA((1,))]
        send_two, keep_two = segment_product(
            build_packed, plan, [grad_rows], [any_spec], row_bufs, col_nodes, 1, blk_nodes)
        back_two = (keep_two + lax.ppermute(send_two, "row", swap)).astype(jnp.bfloat16)
        z_second, back_two = lax.optimization_barrier((z_second, back_two))
        back_all = lax.all_gather(back_two, ("col", "row"), axis=0, tiled=True)
        back_rows = lax.dynamic_slice_in_dim(back_all, row_i * col_size * packed, col_size * packed, 0)
        back_own = lax.dynamic_slice_in_dim(back_rows, col_j * packed, packed, 0)
        back_own = jnp.concatenate([back_own[:, q * pack_lanes():q * pack_lanes() + classes] for q in range(PACK)], axis=0)[:blk_nodes]
        h_one = jnp.maximum(z_one, 0)
        grad_w_output = lax.dot_general(h_one, back_own, CONTRACT_ROWS, preferred_element_type=jnp.float32)

        send_one, keep_one = segment_product(
            build_dz, plan, [z_first, z_second, back_rows, w_out_pad], [any_spec, any_spec, any_spec, whole],
            [pltpu.VMEM((2, 4, 1024, 2 * LANES), jnp.bfloat16), pltpu.SemaphoreType.DMA((2, 4)), *row_bufs,
             pltpu.VMEM((blk_nodes + 128, LANES), jnp.bfloat16)],
            col_nodes, 2, blk_nodes)
        back_one = (keep_one + lax.ppermute(send_one, "row", swap)).astype(jnp.bfloat16)
        feat_src = lax.dynamic_slice_in_dim(x_all, (col_j * row_size + row_i) * blk_nodes, blk_nodes, 0)
        grad_w_hidden = lax.dot_general(feat_src, back_one, CONTRACT_ROWS, preferred_element_type=jnp.float32)
        feat, hid = w_hidden.shape
        out_pad = jnp.pad(grad_w_output, ((0, 0), (0, LANES - classes)))
        rows = feat * hid // LANES + hid
        packed_out = jnp.concatenate([grad_w_hidden.reshape(-1, LANES), out_pad, jnp.full((1, LANES), loss_mean)], axis=0)
        unit = 8 * row_size * col_size
        packed_out = jnp.pad(packed_out, ((0, -(rows + 1) % unit), (0, 0)))
        total = all_reduce(packed_out, row_size, col_size)
        grad_w_hidden = total[:feat * hid // LANES].reshape(feat, hid)
        return total[rows, 0], grad_w_hidden, total[feat * hid // LANES:rows, :classes]

    node_spec = P(("row", "col"), None)
    label_spec = P(("row", "col"))
    adj_spec = P("col", "row")
    return jax.shard_map(device_step, mesh=mesh, in_specs=(node_spec, P(), P(), adj_spec, adj_spec, adj_spec, label_spec, label_spec), out_specs=(P(), P(), P()), check_vma=False)
```

```python
import functools

import jax
import jax.numpy as jnp
from jax import lax
from jax.experimental import pallas as pl
from jax.experimental.pallas import tpu as pltpu
from jax.sharding import PartitionSpec as P


CONTRACT_ROWS = (((0,), (0,)), ((), ()))
CONTRACT_COLS = (((1,), (1,)), ((), ()))
LANES = 128
SUB_ROWS = 256
STEP_SUBS = 4
PIECE_ROWS = 32
PIECES = 8
BUF_SUBS = 1
CHUNK = 256
BUF_CHUNKS = 2
STEP_CHUNKS = 16
WINDOW = 256
PACK = 3
INNER = 4
VMEM = 63 << 20


def copy_row(ids, e, table, stage, at, width):
    if width == 1:
        stage[at, :] = table[ids[e], :]
    else:
        stage[width * at:width * (at + 1), :] = table[pl.ds(pl.multiple_of(ids[e], width), width), :]


def index_copy(idx_hbm, ids, sems, buf, step):
    size = ids[buf].shape[0]
    start = pl.multiple_of((step * len(ids) + buf) * size, size)
    return pltpu.make_async_copy(idx_hbm.at[pl.ds(start, size)], ids[buf], sems.at[buf])


def start_next(idx_hbm, ids, sems, buf, following, total):
    @pl.when(following < total)
    def _():
        index_copy(idx_hbm, ids, sems, buf, following).start()


def store_table(table, first, value, width):
    rows = value.shape[0]
    for part in range(width):
        piece = value[:, part * LANES:(part + 1) * LANES]
        if width == 1:
            table[pl.ds(pl.multiple_of(first, rows), rows), :] = piece
        else:
            table[pl.ds(width * first + part, rows, stride=width), :] = piece


def stream_rows(source, buffer, sems, phase, phases, total, use, shift=0):
    slots, chunk = buffer.shape[0], buffer.shape[1]
    steps = total // chunk
    assert steps % slots == 0

    def copy(step, slot):
        start = pl.multiple_of(shift + phase * total + step * chunk, 16)
        return pltpu.make_async_copy(source.at[pl.ds(start, chunk), :], buffer.at[slot], sems.at[slot])

    @pl.when(phase == 0)
    def _():
        for slot in range(slots):
            copy(slot, slot).start()

    def body(group, carry):
        for slot in range(slots):
            step = group * slots + slot
            copy(step, slot).wait()
            use(buffer.at[slot], step * chunk)

            @pl.when((step + slots < steps) | (phase + 1 < phases))
            def _():
                copy(step + slots, slot).start()
        return carry

    lax.fori_loop(0, steps // slots, body, 0)


def weight_columns(w_ref, first):
    w_rows = w_ref[0, :, pl.ds(pl.multiple_of(first, LANES), LANES)]
    return jnp.concatenate([w_rows] * (8 // w_ref.shape[1]), axis=0).T


def weighted_sum(stage, w_cols, slots, first, size, width):
    parts = [None] * width
    inside = first % LANES
    for slot in range(slots):
        column = jnp.broadcast_to(w_cols[inside:inside + size, slot:slot + 1], (size, LANES))
        at = width * (slot * SUB_ROWS + first)
        for part in range(width):
            rows = stage[pl.ds(at + part, size, stride=width), :] if width > 1 else stage[at:at + size, :]
            term = column * rows
            parts[part] = term if slot == 0 else parts[part] + term
    return parts


def forward_step(idx_hbm, w_ref, table, acc, ids, stages, idx_sems, width):
    phase, tile = pl.program_id(0), pl.program_id(1)
    per_phase = pl.num_programs(1) * INNER
    total = pl.num_programs(0) * per_phase
    slots = w_ref.shape[1]
    edges = slots * SUB_ROWS
    pieces = SUB_ROWS // PIECE_ROWS
    step_rows = STEP_SUBS * SUB_ROWS

    @pl.when((phase == 0) & (tile == 0))
    def _():
        for buf in range(len(ids)):
            index_copy(idx_hbm, ids, idx_sems, buf, 0).start()

    def inner(n, carry):
        step = phase * per_phase + tile * INNER + n
        first_row = pl.multiple_of((tile * INNER + n) * step_rows, step_rows)

        @pl.when(phase == 0)
        def _():
            acc[pl.ds(first_row, step_rows), :] = jnp.zeros((step_rows, acc.shape[1]), jnp.float32)

        for sub in range(STEP_SUBS + 1):
            buf, part = sub // BUF_SUBS, sub % BUF_SUBS
            if part == 0 and sub < STEP_SUBS:
                index_copy(idx_hbm, ids, idx_sems, buf, step).wait()
            for piece in range(pieces):
                first = piece * PIECE_ROWS
                if sub > 0 and first % LANES == 0:
                    w_cols = weight_columns(w_ref, n * step_rows + (sub - 1) * SUB_ROWS + first)
                if sub < STEP_SUBS:
                    for e in range(piece * edges // pieces, (piece + 1) * edges // pieces):
                        copy_row(ids[buf], part * edges + e, table, stages[sub % len(stages)], e, width)
                if sub > 0:
                    parts = weighted_sum(stages[(sub - 1) % len(stages)], w_cols, slots, first, PIECE_ROWS, width)
                    rows = pl.ds(pl.multiple_of(first_row + (sub - 1) * SUB_ROWS + first, PIECE_ROWS), PIECE_ROWS)
                    for lane in range(width):
                        acc[rows, lane * LANES:(lane + 1) * LANES] += parts[lane]
            if part == BUF_SUBS - 1 and sub < STEP_SUBS:
                start_next(idx_hbm, ids, idx_sems, buf, step + 1, total)
        return carry

    lax.fori_loop(0, INNER, inner, 0)


def finish_rows(acc, use):
    tile = pl.program_id(1)
    size = INNER * STEP_SUBS * SUB_ROWS

    def body(n, carry):
        at = pl.multiple_of(n * 256, 256)
        use(pl.ds(at, 256), acc[pl.ds(pl.multiple_of(tile * size + at, 256), 256), :])
        return carry

    lax.fori_loop(0, size // 256, body, 0)


def layer_one_kernel(idx_hbm, w_ref, x_hbm, w_hidden, w_output, z_ref, p_ref, table, acc, ids_a, ids_b, ids_c, ids_d, stage_a, stage_b, x_buf,
                     sems, idx_sems):
    phase, tile = pl.program_id(0), pl.program_id(1)
    col_nodes = table.shape[0] // 2

    @pl.when(tile == 0)
    def _():
        def use(buf, offset):
            def body(n, carry):
                for part in range(2):
                    sub = pl.multiple_of(n * 512 + part * 256, 256)
                    proj = jnp.dot(buf[pl.ds(sub, 256), :], w_hidden[...], preferred_element_type=jnp.float32)
                    proj = proj.astype(jnp.bfloat16).astype(jnp.float32)
                    store_table(table, offset + sub, proj, 2)
                return carry

            lax.fori_loop(0, x_buf.shape[1] // 512, body, 0)

        stream_rows(x_hbm, x_buf, sems, phase, pl.num_programs(0), col_nodes, use)

    forward_step(idx_hbm, w_ref, table, acc, [ids_a, ids_b, ids_c, ids_d], [stage_a, stage_b], idx_sems, 2)

    @pl.when(phase == pl.num_programs(0) - 1)
    def _():
        def use(at, sums):
            z_one = sums.astype(jnp.bfloat16)
            z_ref[at, :] = z_one
            h_one = jnp.maximum(z_one, 0)
            p_ref[at, :] = jnp.dot(h_one, w_output[...], preferred_element_type=jnp.float32).astype(jnp.bfloat16)

        finish_rows(acc, use)


def unpack_table(table, p_hbm, p_buf, sems, phase, phases, blocks, nodes, first_block=0):
    packed = packed_rows(nodes)
    piece = packed // 18

    def use(buf, offset):
        block = offset // packed

        def body(n, carry):
            inside = pl.multiple_of(n * piece, 16)
            value = buf[pl.ds(inside, piece), :].astype(jnp.float32)
            for q in range(PACK):
                turned = value if q == 0 else pltpu.roll(value, LANES - q * pack_lanes(), 1)
                first = pl.multiple_of(block * nodes + q * packed + inside, 16)
                table[pl.ds(first, piece), :] = turned.astype(table.dtype)
            return carry

        lax.fori_loop(0, 18, body, 0)

    stream_rows(p_hbm, p_buf, sems, phase, phases, blocks * packed, use, first_block * packed)


def pack_lanes():
    return LANES // PACK // 8 * 8


def packed_rows(nodes):
    return -(-nodes // (PACK * 96)) * 96


def pack_nodes(values):
    nodes = values.shape[0]
    packed = packed_rows(nodes)
    values = jnp.pad(values, ((0, PACK * packed - nodes), (0, pack_lanes() - values.shape[1])))
    parts = [values[q * packed:(q + 1) * packed] for q in range(PACK)]
    return jnp.pad(jnp.concatenate(parts, axis=1), ((0, 0), (0, LANES - PACK * pack_lanes())))


def pack_rows(acc, first, piece, packed, n):
    lane = lax.broadcasted_iota(jnp.int32, (piece, LANES), 1)
    total = None
    for q in range(PACK):
        rows = acc[pl.ds(pl.multiple_of(first + q * packed + n * piece, 8), piece), :]
        rows = jnp.where(lane < pack_lanes(), rows, 0.0)
        rows = rows if q == 0 else pltpu.roll(rows, q * pack_lanes(), 1)
        total = rows if q == 0 else total + rows
    return total


def layer_two_kernel(nodes, classes, idx_hbm, w_ref, p_hbm, node_ref, count_ref, grad_ref, loss_ref, table, acc, ids_a, ids_b,
                     ids_c, ids_d, stage_a, stage_b, p_buf, sems, idx_sems):
    phase, tile = pl.program_id(0), pl.program_id(1)
    packed = packed_rows(nodes)

    @pl.when((phase == 0) & (tile == 0))
    def _():
        acc[nodes:, :] = jnp.zeros((acc.shape[0] - nodes, LANES), jnp.float32)
        loss_ref[...] = jnp.zeros_like(loss_ref)

    @pl.when(tile == 0)
    def _():
        unpack_table(table, p_hbm, p_buf, sems, phase, pl.num_programs(0), 2, nodes)

    forward_step(idx_hbm, w_ref, table, acc, [ids_a, ids_b, ids_c, ids_d], [stage_a, stage_b], idx_sems, 1)

    @pl.when(phase == pl.num_programs(0) - 1)
    def _():
        size = INNER * STEP_SUBS * SUB_ROWS
        group = 512
        lane = lax.broadcasted_iota(jnp.int32, (group, LANES), 1)
        lane_f = lane.astype(jnp.float32)
        count = count_ref[0]

        def body(n, carry):
            rows = pl.ds(pl.multiple_of(tile * size + n * group, group), group)
            columns = node_ref[:, rows].T
            label = jnp.broadcast_to(columns[:, 0:1], (group, LANES))
            mask = jnp.broadcast_to(columns[:, 1:2], (group, LANES))
            z_two = jnp.where(lane < classes, acc[rows, :], -jnp.inf)
            top = jnp.max(z_two, axis=1, keepdims=True)
            log_norm = jnp.log(jnp.sum(jnp.exp(z_two - top), axis=1, keepdims=True)) + top
            hit = lane_f == label
            terms = mask * (jnp.where(lane == 0, log_norm, 0.0) - jnp.where(hit, z_two, 0.0))
            loss_ref[...] += jnp.sum(terms.reshape(group // 8, 8, LANES), axis=0)
            acc[rows, :] = (mask / count) * (jnp.exp(z_two - log_norm) - jnp.where(hit, 1.0, 0.0))
            return carry

        lax.fori_loop(0, size // group, body, 0)

    @pl.when((phase == pl.num_programs(0) - 1) & (tile == pl.num_programs(1) - 1))
    def _():
        piece = packed // 18

        def body(n, carry):
            grad_ref[pl.ds(pl.multiple_of(n * piece, 16), piece), :] = pack_rows(acc, 0, piece, packed, n).astype(jnp.bfloat16)
            return carry

        lax.fori_loop(0, 18, body, 0)


def segment_kernel(width, nodes, n_src, build, active_ref, over_ref, base_ref, last_ref, idx_hbm, col_ref, w_ref, *refs):
    bufs = STEP_CHUNKS // BUF_CHUNKS
    sources, refs = refs[:n_src], refs[n_src:]
    (out_first, out_second, table, acc, spare_ids, stage_a, stage_b, idx_sems, spare_sem, out_sems), refs = refs[:10], refs[10:]
    ids, refs = refs[:bufs], refs[bufs:]
    if width == 1:
        packed_sums, refs = refs[0], refs[1:]
    buffers, sems = refs[0::2], refs[1::2]
    stages = [stage_a, stage_b]
    phases = active_ref.shape[0] - 1
    phase, tile = pl.program_id(0), pl.program_id(1)
    steps = pl.num_programs(1) * INNER
    total = pl.num_programs(0) * steps

    @pl.when((phase == 0) & (tile == 0))
    def _():
        for buf in range(len(ids)):
            index_copy(idx_hbm, ids, idx_sems, buf, 0).start()

        def zero(n, carry):
            acc[pl.ds(pl.multiple_of(n * 256, 256), 256), :] = jnp.zeros((256, acc.shape[1]), jnp.float32)
            return carry

        lax.fori_loop(0, acc.shape[0] // 256, zero, 0)

    @pl.when(tile == 0)
    def _():
        build(sources, buffers, sems, phase, pl.num_programs(0), active_ref[phases], table)

    def gathered(stage):
        lanes = []
        for part in range(width):
            rows = stage[pl.ds(part, CHUNK, stride=width), :] if width > 1 else stage[...]
            lanes.append(rows.astype(jnp.bfloat16))
        return jnp.concatenate(lanes, axis=1) if width > 1 else lanes[0]

    def product(cols, weights, rows, base):
        local = lax.broadcasted_iota(jnp.int32, (WINDOW, CHUNK), 0)
        select = jnp.where(local == cols - base, weights, 0.0).astype(jnp.bfloat16)
        acc[pl.ds(pl.multiple_of(base, 8), WINDOW), :] += jnp.dot(select, rows, preferred_element_type=jnp.float32)

    def inner(n, carry):
        place = tile * INNER + n
        step = phase * steps + place
        following = jnp.where(place + 1 < active_ref[phase], step + 1, (phase + 1) * steps)

        def lanes_of(chunk):
            return pl.ds(pl.multiple_of((n * STEP_CHUNKS + chunk) * CHUNK, CHUNK), CHUNK)

        def multiply(chunk):
            part = lanes_of(chunk)
            base = base_ref[step * STEP_CHUNKS + chunk]
            local = lax.broadcasted_iota(jnp.int32, (WINDOW, CHUNK), 0)
            select = jnp.where(local == col_ref[0, :, part] - base, w_ref[0, :, part], 0.0).astype(jnp.bfloat16)
            return base, jnp.dot(select, gathered(stages[chunk % 2]), preferred_element_type=jnp.float32)

        size = WINDOW // PIECES
        for chunk in range(STEP_CHUNKS + 1):
            buf, part = chunk // BUF_CHUNKS, chunk % BUF_CHUNKS
            if part == 0 and chunk < STEP_CHUNKS:
                index_copy(idx_hbm, ids, idx_sems, buf, step).wait()
            if chunk > 0:
                base, sums = multiply(chunk - 1)
            for piece in range(PIECES):
                if chunk < STEP_CHUNKS:
                    for e in range(piece * CHUNK // PIECES, (piece + 1) * CHUNK // PIECES):
                        copy_row(ids[buf], part * CHUNK + e, table, stages[chunk % 2], e, width)
                if chunk > 0:
                    at = pl.ds(pl.multiple_of(base + piece * size, 8), size)
                    acc[at, :] += sums[piece * size:(piece + 1) * size, :]
            if part == BUF_CHUNKS - 1 and chunk < STEP_CHUNKS:
                start_next(idx_hbm, ids, idx_sems, buf, following, total)

        @pl.when(over_ref[step] > 0)
        def _():
            wide_chunks(n, step)

        return carry

    def wide_chunks(n, step):
        size = STEP_CHUNKS * CHUNK
        copy = pltpu.make_async_copy(idx_hbm.at[pl.ds(pl.multiple_of(step * size, size), size)], spare_ids, spare_sem)
        copy.start()
        copy.wait()

        def wide(chunk, carry):
            base, last = base_ref[step * STEP_CHUNKS + chunk], last_ref[step * STEP_CHUNKS + chunk]

            @pl.when(last >= base + WINDOW)
            def _():
                def fetch(e, carry):
                    copy_row(spare_ids, chunk * CHUNK + e, table, stage_a, 0, width)
                    if width == 1:
                        stage_b[pl.ds(e, 1), :] = stage_a[0:1, :]
                    else:
                        stage_b[pl.ds(width * e, width), :] = stage_a[0:width, :]
                    return carry

                lax.fori_loop(0, CHUNK, fetch, 0)
                part = pl.ds(pl.multiple_of((n * STEP_CHUNKS + chunk) * CHUNK, CHUNK), CHUNK)
                cols, weights = col_ref[0, :, part], w_ref[0, :, part]
                rows = gathered(stage_b)
                end = acc.shape[0] - WINDOW

                def more(window, carry):
                    start = base + window * WINDOW
                    fresh = jnp.where(cols >= start, weights, 0.0)
                    product(cols, fresh, rows, jnp.minimum(start, end))
                    return carry

                lax.fori_loop(1, (last - base) // WINDOW + 1, more, 0)

            return carry

        lax.fori_loop(0, STEP_CHUNKS, wide, 0)

    lax.fori_loop(0, jnp.clip(active_ref[phase] - tile * INNER, 0, INNER), inner, 0)

    @pl.when((phase == pl.num_programs(0) - 1) & (tile == pl.num_programs(1) - 1))
    def _():
        half = nodes
        if width == 1:
            packed = packed_rows(nodes)
            piece = packed // 18
            for part in range(2):
                def body(n, carry):
                    at = pl.ds(pl.multiple_of(n * piece, 8), piece)
                    packed_sums[part, at, :] = pack_rows(acc, part * half, piece, packed, n)
                    return carry

                lax.fori_loop(0, 18, body, 0)
            results = [packed_sums.at[0], packed_sums.at[1]]
        else:
            results = [acc.at[pl.ds(part * half, half), :] for part in range(2)]
        copies = [pltpu.make_async_copy(result, out, out_sems.at[n])
                  for n, (result, out) in enumerate(zip(results, [out_first, out_second]))]
        for copy in copies:
            copy.start()
        for copy in copies:
            copy.wait()


def build_packed(nodes, sources, buffers, sems, phase, phases, first_block, table):
    unpack_table(table, sources[0], buffers[0], sems[0], phase, phases, 1, nodes)


def build_dz(nodes, sources, buffers, sems, phase, phases, first_block, table):
    z_first, z_second, b_hbm, w_out = sources
    z_buf, b_buf, back = buffers
    half = nodes // 2
    unpack_table(back, b_hbm, b_buf, sems[1], phase, phases, 1, nodes, first_block)

    def use(buf, offset):
        for sub in range(0, z_buf.shape[2], 256):
            z_one = buf[sub:sub + 256, :]
            back_two = back[pl.ds(pl.multiple_of(offset + sub, 256), 256), :]
            dh_one = lax.dot_general(back_two, w_out[...], CONTRACT_COLS, preferred_element_type=jnp.float32)
            dz_one = jnp.where(z_one.astype(jnp.float32) > 0, dh_one, 0.0).astype(jnp.bfloat16)
            store_table(table, offset + sub, dz_one.astype(jnp.float32), 2)

    stream_rows(z_first, z_buf.at[0], sems[0].at[0], phase, phases, half, use)
    stream_rows(z_second, z_buf.at[1], sems[0].at[1], phase, phases, half, lambda buf, offset: use(buf, half + offset))


def params():
    return pltpu.CompilerParams(vmem_limit_bytes=VMEM, dimension_semantics=("arbitrary", "arbitrary"))


def forward_specs(weights, last):
    slots = weights.shape[1]
    rows = INNER * STEP_SUBS * SUB_ROWS
    w_spec = pl.BlockSpec((1, slots, rows), lambda k, t: (k, 0, t))

    def out_spec(width):
        return pl.BlockSpec((rows, width), lambda k, t: (jnp.where(k == last, t, 0), 0))

    ids = pltpu.SMEM((BUF_SUBS * slots * SUB_ROWS,), jnp.int32)
    return w_spec, out_spec, [ids] * (STEP_SUBS // BUF_SUBS)


def layer_one(idx, weights, x_all, w_hidden, w_out_pad):
    phases, slots, rows = weights.shape
    nodes, feat = x_all.shape
    hid = w_hidden.shape[1]
    whole = pl.BlockSpec(memory_space=pltpu.VMEM)
    any_spec = pl.BlockSpec(memory_space=pl.ANY)
    w_spec, out_spec, ids = forward_specs(weights, phases - 1)
    stage = pltpu.VMEM((2 * slots * SUB_ROWS, LANES), jnp.float32)
    return pl.pallas_call(
        layer_one_kernel,
        grid=(phases, rows // (INNER * STEP_SUBS * SUB_ROWS)),
        in_specs=[any_spec, w_spec, any_spec, whole, whole],
        out_specs=[out_spec(hid), out_spec(LANES)],
        out_shape=[jax.ShapeDtypeStruct((rows, hid), jnp.bfloat16), jax.ShapeDtypeStruct((rows, LANES), jnp.bfloat16)],
        scratch_shapes=[
            pltpu.VMEM((2 * nodes // phases, LANES), jnp.float32), pltpu.VMEM((rows, hid), jnp.float32),
            *ids, stage, stage, pltpu.VMEM((2, 4096, feat), jnp.bfloat16),
            pltpu.SemaphoreType.DMA((2,)), pltpu.SemaphoreType.DMA((STEP_SUBS // BUF_SUBS,))],
        compiler_params=params(),
        cost_estimate=pl.CostEstimate(flops=2 * 10**11, bytes_accessed=10**8, transcendentals=0),
        name="layer_one")(idx, weights, x_all, w_hidden, w_out_pad)


def layer_two(idx, weights, p_all, node_rows, count, classes):
    phases, slots, rows = weights.shape
    any_spec = pl.BlockSpec(memory_space=pl.ANY)
    whole = pl.BlockSpec(memory_space=pltpu.VMEM)
    w_spec, _, ids = forward_specs(weights, phases - 1)
    stage = pltpu.VMEM((slots * SUB_ROWS, LANES), jnp.float32)
    return pl.pallas_call(
        functools.partial(layer_two_kernel, rows, classes),
        grid=(phases, rows // (INNER * STEP_SUBS * SUB_ROWS)),
        in_specs=[any_spec, w_spec, any_spec, whole, pl.BlockSpec(memory_space=pltpu.SMEM)],
        out_specs=[whole, whole],
        out_shape=[jax.ShapeDtypeStruct((packed_rows(rows), LANES), jnp.bfloat16), jax.ShapeDtypeStruct((8, LANES), jnp.float32)],
        scratch_shapes=[
            pltpu.VMEM((2 * rows + 128, LANES), jnp.float32), pltpu.VMEM((rows + 128, LANES), jnp.float32),
            *ids, stage, stage, pltpu.VMEM((2, packed_rows(rows), LANES), jnp.bfloat16),
            pltpu.SemaphoreType.DMA((2,)), pltpu.SemaphoreType.DMA((STEP_SUBS // BUF_SUBS,))],
        compiler_params=params(),
        cost_estimate=pl.CostEstimate(flops=2 * 10**11, bytes_accessed=10**8, transcendentals=0),
        name="layer_two")(idx, weights, p_all, node_rows, count)


def segment_product(build, plan, sources, specs, buffers, num_out, width, rows):
    ids_by_width, cols, weights, scalars = plan
    phases = scalars[0].shape[0] - 1
    steps, per_step = cols.shape[0] // phases, cols.shape[2]
    any_spec = pl.BlockSpec(memory_space=pl.ANY)
    tile_spec = pl.BlockSpec((1, 1, per_step), lambda p, t, *_: (p * steps + t, 0, 0))
    ids = pltpu.SMEM((BUF_CHUNKS * CHUNK,), jnp.int32)
    stage = pltpu.VMEM((width * CHUNK, LANES), jnp.float32)
    out_rows = packed_rows(rows) if width == 1 else num_out // 2
    sums = [pltpu.VMEM((2, out_rows, LANES), jnp.float32)] if width == 1 else []
    grid_spec = pltpu.PrefetchScalarGridSpec(
        num_scalar_prefetch=len(scalars),
        grid=(phases, steps),
        in_specs=[any_spec, tile_spec, tile_spec, *specs],
        out_specs=[any_spec, any_spec],
        scratch_shapes=[
            pltpu.VMEM((width * rows + (128 if width == 1 else 0), LANES), jnp.float32),
            pltpu.VMEM((num_out + (256 if width == 1 else 0), width * LANES), jnp.float32),
            pltpu.SMEM((STEP_CHUNKS * CHUNK,), jnp.int32), stage, stage,
            pltpu.SemaphoreType.DMA((STEP_CHUNKS // BUF_CHUNKS,)), pltpu.SemaphoreType.DMA, pltpu.SemaphoreType.DMA((2,)),
            *([ids] * (STEP_CHUNKS // BUF_CHUNKS)), *sums, *buffers])
    return pl.pallas_call(
        functools.partial(segment_kernel, width, rows, len(sources), functools.partial(build, rows)),
        grid_spec=grid_spec,
        out_shape=[jax.ShapeDtypeStruct((out_rows, width * LANES), jnp.float32)] * 2,
        compiler_params=params(),
        cost_estimate=pl.CostEstimate(flops=2 * 10**11, bytes_accessed=10**8, transcendentals=0))(*scalars, ids_by_width[width - 1], cols, weights, *sources)


def edge_lists(cols_blk, mask_blk, vals_blk, col_blocks, blk_nodes, turn):
    slots = cols_blk.shape[0]
    col_nodes = 2 * blk_nodes
    row_ids = lax.broadcasted_iota(jnp.int32, (slots, col_blocks, blk_nodes), 2)
    valid = mask_blk.reshape(slots, col_blocks, blk_nodes) > 0
    turned = jnp.bitwise_xor(cols_blk, turn).reshape(slots, col_blocks, blk_nodes)
    keys = jnp.where(valid, turned, col_nodes) * blk_nodes + row_ids
    weights = jnp.where(valid, vals_blk.reshape(slots, col_blocks, blk_nodes).astype(jnp.float32), 0.0)
    keys = keys.transpose(1, 0, 2).reshape(col_blocks, slots * blk_nodes)
    return keys, weights.transpose(1, 0, 2).reshape(col_blocks, slots * blk_nodes)


def make_plan(keys, weights, blk_nodes, first_block):
    col_nodes = 2 * blk_nodes
    cols, rows = keys // blk_nodes, keys % blk_nodes
    chunked = cols.reshape(-1, CHUNK)
    base = jnp.minimum(chunked[:, 0] // 8 * 8, col_nodes - WINDOW)
    last = jnp.max(jnp.where(chunked < col_nodes, chunked, -1), axis=1)
    over = jnp.max((last >= base + WINDOW).astype(jnp.int32).reshape(-1, STEP_CHUNKS), axis=1)
    count = jnp.sum((cols < col_nodes).astype(jnp.int32), axis=1)
    active = jnp.maximum((count + STEP_CHUNKS * CHUNK - 1) // (STEP_CHUNKS * CHUNK), 1)
    active = jnp.concatenate([active, first_block.reshape(1)])
    tiles = (-1, 1, INNER * STEP_CHUNKS * CHUNK)
    ids_by_width = (rows.reshape(-1), 2 * rows.reshape(-1))
    return ids_by_width, cols.reshape(tiles), weights.reshape(tiles), (active, over, base, last)


def all_reduce_kernel(row_size, col_size, x_ref, out_ref, held, send_a, recv_a, send_b, recv_b):
    devices = row_size * col_size
    me = lax.axis_index("row") * col_size + lax.axis_index("col")
    size = x_ref.shape[0] // devices

    def place(index):
        return {"row": index // col_size, "col": index % col_size}

    barrier = pltpu.get_barrier_semaphore()
    for d in range(1, devices):
        pl.semaphore_signal(barrier, inc=1, device_id=place((me + d) % devices), device_id_type=pl.DeviceIdType.MESH)
    pl.semaphore_wait(barrier, devices - 1)
    copies = []
    for d in range(1, devices):
        peer = (me + d) % devices
        copies.append(pltpu.make_async_remote_copy(
            src_ref=x_ref.at[pl.ds(pl.multiple_of(peer * size, size), size), :], dst_ref=held.at[d - 1],
            send_sem=send_a.at[d - 1], recv_sem=recv_a.at[d - 1], device_id=place(peer), device_id_type=pl.DeviceIdType.MESH))
    for copy in copies:
        copy.start()
    for copy in copies:
        copy.wait()
    mine = pl.ds(pl.multiple_of(me * size, size), size)
    total = x_ref[mine, :]
    for d in range(1, devices):
        total = total + held[d - 1]
    out_ref[mine, :] = total
    copies = []
    for d in range(1, devices):
        copies.append(pltpu.make_async_remote_copy(
            src_ref=out_ref.at[mine, :], dst_ref=out_ref.at[mine, :], send_sem=send_b.at[d - 1], recv_sem=recv_b.at[d - 1],
            device_id=place((me + d) % devices), device_id_type=pl.DeviceIdType.MESH))
    for copy in copies:
        copy.start()
    for copy in copies:
        copy.wait()


def all_reduce(x, row_size, col_size):
    devices = row_size * col_size
    whole = pl.BlockSpec(memory_space=pltpu.VMEM)
    sems = pltpu.SemaphoreType.DMA((devices - 1,))
    return pl.pallas_call(
        functools.partial(all_reduce_kernel, row_size, col_size),
        in_specs=[whole],
        out_specs=whole,
        out_shape=jax.ShapeDtypeStruct(x.shape, x.dtype),
        scratch_shapes=[pltpu.VMEM((devices - 1, x.shape[0] // devices, x.shape[1]), x.dtype), sems, sems, sems, sems],
        compiler_params=pltpu.CompilerParams(collective_id=0, has_side_effects=True),
        name="all_reduce")(x)


def solution(mesh):
    row_size = mesh.shape["row"]
    col_size = mesh.shape["col"]
    both_axes = ("row", "col")
    swap = [(0, 1), (1, 0)]

    def device_step(feat_blk, w_hidden, w_output, cols_blk, vals_blk, mask_blk, labels_blk, train_blk):
        row_i, col_j = lax.axis_index("row"), lax.axis_index("col")
        blk_nodes = feat_blk.shape[0]
        col_nodes = blk_nodes * row_size
        packed = packed_rows(blk_nodes)
        slots = cols_blk.shape[0]
        classes = w_output.shape[1]
        any_spec = pl.BlockSpec(memory_space=pl.ANY)
        whole = pl.BlockSpec(memory_space=pltpu.VMEM)
        w_out_pad = jnp.pad(w_output, ((0, 0), (0, LANES - classes)))

        x_all = lax.all_gather(feat_blk, both_axes, axis=0, tiled=True)
        masked = vals_blk * mask_blk.astype(jnp.bfloat16)
        own_cols = lax.all_to_all(cols_blk, "col", split_axis=1, concat_axis=0, tiled=True)
        own_w = lax.all_to_all(masked, "col", split_axis=1, concat_axis=0, tiled=True)
        own_w = own_w.astype(jnp.float32).reshape(col_size, slots, blk_nodes)
        own_cols = own_cols.reshape(col_size, slots, -1, STEP_SUBS, SUB_ROWS).transpose(0, 2, 3, 1, 4).reshape(-1)

        keys, edge_w = edge_lists(cols_blk, mask_blk, vals_blk, col_size, blk_nodes, (1 - row_i) * blk_nodes)
        edges = lax.sort((keys, edge_w), dimension=1, num_keys=1, is_stable=False)
        x_all, edges = lax.optimization_barrier((x_all, edges))
        plan = make_plan(*edges, blk_nodes, row_i * col_size)

        z_one, proj_two = layer_one(own_cols * 2, own_w, x_all, w_hidden, w_out_pad)
        count = jnp.sum(train_blk)
        spare = PACK * pack_lanes()
        lane_ids = lax.broadcasted_iota(jnp.int32, (packed, LANES), 1)
        counts = jnp.where(lane_ids == spare, count // 128, jnp.where(lane_ids == spare + 1, count % 128, 0))
        p_all = lax.all_gather(pack_nodes(proj_two[:, :classes]) + counts.astype(jnp.bfloat16), both_axes, axis=0, tiled=True)
        feat_src = lax.dynamic_slice_in_dim(x_all, (col_j * row_size + row_i) * blk_nodes, blk_nodes, 0)
        z_one, p_all, plan, feat_src = lax.optimization_barrier((z_one, p_all, plan, feat_src))
        z_first = lax.all_gather(z_one[:blk_nodes // 2], "col", axis=0, tiled=True)
        counts = p_all.reshape(row_size * col_size, packed, LANES)[:, 0, spare:spare + 2].astype(jnp.float32)
        train_count = jnp.maximum(jnp.sum(counts[:, 0] * 128.0 + counts[:, 1]), 1.0)
        node_rows = jnp.zeros((8, blk_nodes), jnp.float32)
        node_rows = node_rows.at[0].set(labels_blk.astype(jnp.float32)).at[1].set(train_blk.astype(jnp.float32))
        grad_two, loss = layer_two(own_cols, own_w, p_all, node_rows, train_count.reshape(1), classes)
        loss_mean = jnp.sum(loss) / train_count
        z_first, grad_two = lax.optimization_barrier((z_first, grad_two))
        grad_rows = lax.all_gather(grad_two, "col", axis=0, tiled=True)
        z_later, grad_rows = lax.optimization_barrier((z_one[blk_nodes // 2:], grad_rows))
        z_second = lax.all_gather(z_later, "col", axis=0, tiled=True)

        row_bufs = [pltpu.VMEM((1, packed, LANES), jnp.bfloat16), pltpu.SemaphoreType.DMA((1,))]
        send_two, keep_two = segment_product(
            build_packed, plan, [grad_rows], [any_spec], row_bufs, col_nodes, 1, blk_nodes)
        back_two = (keep_two + lax.ppermute(send_two, "row", swap)).astype(jnp.bfloat16)
        z_second, back_two = lax.optimization_barrier((z_second, back_two))
        back_all = lax.all_gather(back_two, ("col", "row"), axis=0, tiled=True)
        back_own = lax.dynamic_slice_in_dim(back_all, (row_i * col_size + col_j) * packed, packed, 0)
        back_own = jnp.concatenate([back_own[:, q * pack_lanes():q * pack_lanes() + classes] for q in range(PACK)], axis=0)[:blk_nodes]
        h_one = jnp.maximum(z_one, 0)
        grad_w_output = lax.dot_general(h_one, back_own, CONTRACT_ROWS, preferred_element_type=jnp.float32)

        send_one, keep_one = segment_product(
            build_dz, plan, [z_first, z_second, back_all, w_out_pad], [any_spec, any_spec, any_spec, whole],
            [pltpu.VMEM((2, 4, 1024, 2 * LANES), jnp.bfloat16), pltpu.SemaphoreType.DMA((2, 4)), *row_bufs,
             pltpu.VMEM((blk_nodes + 128, LANES), jnp.bfloat16)],
            col_nodes, 2, blk_nodes)
        back_one = (keep_one + lax.ppermute(send_one, "row", swap)).astype(jnp.bfloat16)
        grad_w_hidden = lax.dot_general(feat_src, back_one, CONTRACT_ROWS, preferred_element_type=jnp.float32)
        feat, hid = w_hidden.shape
        out_pad = jnp.pad(grad_w_output, ((0, 0), (0, LANES - classes)))
        rows = feat * hid // LANES + hid
        packed_out = jnp.concatenate([grad_w_hidden.reshape(-1, LANES), out_pad, jnp.full((1, LANES), loss_mean)], axis=0)
        unit = 8 * row_size * col_size
        packed_out = jnp.pad(packed_out, ((0, -(rows + 1) % unit), (0, 0)))
        total = all_reduce(packed_out, row_size, col_size)
        grad_w_hidden = total[:feat * hid // LANES].reshape(feat, hid)
        return total[rows, 0], grad_w_hidden, total[feat * hid // LANES:rows, :classes]

    node_spec = P(("row", "col"), None)
    label_spec = P(("row", "col"))
    adj_spec = P("col", "row")
    return jax.shard_map(device_step, mesh=mesh, in_specs=(node_spec, P(), P(), adj_spec, adj_spec, adj_spec, label_spec, label_spec), out_specs=(P(), P(), P()), check_vma=False)
```
